32 devices in a mesh: grp: 2 (over y), tm: 4 (over z), chan: 2 (over x), sub: 2 (over core).
Axes of the slice: x: 2, y: 2, z: 4, core: 2. Of those that a mesh axis runs over, the one named last changes fastest.
Arguments:
- signal: float32 [64, 131072], P(('grp', 'chan', 'sub'), 'tm'), parts along dimension 0, may hold values from -24 to 24
- gap_mask: int32 [64, 8], P(('grp', 'chan', 'sub'), 'tm'), parts along dimension 0, may hold values from 0 to 1, as said below
- assignment: int32 [64], P(('grp', 'chan', 'sub')), parts along dimension 0, may hold values from 0 to 7, as said below
Outputs:
- peak_hold: float32 [64, 16384], P(('grp', 'chan', 'sub'), 'tm'), parts along dimension 0
- log_mean: float32 [64, 16384], P(('grp', 'chan', 'sub'), 'tm'), parts along dimension 0
- block_mean: float32 [16, 16384], P('grp', 'tm'), parts along dimension 0
The draws below stay inside these ranges and needn't reach their ends.
There are 2 independent parts, one for each index of `grp`. The reference program is written for one: setup_inputs(seed, part) draws one part's arguments, and reference() takes and returns one part's arrays. A program takes and returns all parts, laid end to end along the dimension named above; each array names one. Nothing has to cross between parts.
Inputs may be any that keep to these rules, and one draw needn't show every extreme that they name: `gap_mask`: every channel keeps at least one of its 8 segments. `assignment`: every block holds at least one channel.
All inputs are finite; a program needn't handle non-finite values.
Results may differ from the reference program's by a relative error of at most 0.000086.
Values sent between devices are 32-bit elements; how exact they have to be, the bound alone decides.
A program may use at most 128 MiB of HBM per device.

```python
import math
import jax
import jax.numpy as jnp
from jax import lax

LA = 256
LB = 128
BLOCKS = 8
CHANNELS = 32
SEGS = 8
TOTAL = 131072


def draw_signal(key, part):
    base_key = jax.random.fold_in(key, 11)
    noise_key, scale_key, level_key = jax.random.split(base_key, 3)
    noise = jnp.clip(jax.random.normal(noise_key, (CHANNELS, TOTAL), jnp.float32), -6.0, 6.0)
    scales = jnp.exp(jax.random.uniform(scale_key, (CHANNELS, 1), jnp.float32, jnp.log(0.5), jnp.log(2.0)))
    levels = jnp.exp(jax.random.uniform(level_key, (CHANNELS, SEGS), jnp.float32, jnp.log(0.5), jnp.log(2.0)))
    levels = jnp.repeat(levels, LA * LB // 2, axis=1)
    return (noise * scales * levels).astype(jnp.float32)


def draw_gap_mask(key, part):
    base_key = jax.random.fold_in(key, 23)
    rate_key, roll_key, forced_key = jax.random.split(base_key, 3)
    rates = jax.random.randint(rate_key, (CHANNELS, 1), 30, 96)
    rolls = jax.random.randint(roll_key, (CHANNELS, SEGS), 0, 100)
    forced = jax.random.randint(forced_key, (CHANNELS,), 0, SEGS)
    keep_flags = (rolls < rates) | (jnp.arange(SEGS)[None, :] == forced[:, None])
    return keep_flags.astype(jnp.int32)


def draw_assignment(key, part):
    base_key = jax.random.fold_in(key, 37)
    perm_key, pick_key = jax.random.split(base_key, 2)
    order = jax.random.permutation(perm_key, CHANNELS)
    picks = jax.random.randint(pick_key, (CHANNELS,), 0, BLOCKS)
    return picks.at[order[:BLOCKS]].set(jnp.arange(BLOCKS, dtype=jnp.int32)).astype(jnp.int32)


def setup_inputs(seed: int = 0, part: int = 0) -> dict:
    key_of = jax.random.split(jax.random.key(seed), 4)
    own_keys = jax.random.split(jax.random.fold_in(key_of[3], part), 4)
    signal = draw_signal(jax.random.fold_in(jax.random.fold_in(key_of[3], part), 71), part)
    gap_mask = draw_gap_mask(jax.random.fold_in(jax.random.fold_in(key_of[3], part), 71), part)
    assignment = draw_assignment(jax.random.fold_in(jax.random.fold_in(key_of[3], part), 71), part)
    return dict(signal=signal, gap_mask=gap_mask, assignment=assignment)


def reference(signal, gap_mask, assignment):
    seg_length = LA * LB
    half = seg_length // 2
    padded = jnp.concatenate([signal, jnp.zeros((CHANNELS, half), jnp.float32)], 1)
    hop_rows = padded.reshape(CHANNELS, SEGS + 1, half)
    samples = jnp.arange(seg_length)
    window = 0.5 - 0.5 * jnp.cos(2.0 * math.pi * samples / seg_length)
    norm_scale = 1.0 / (0.375 * seg_length)

    def one_channel(inputs):
        rows_here, keep_flags = inputs
        segments = jnp.concatenate([rows_here[:-1], rows_here[1:]], axis=-1) * window
        spectra = jnp.fft.fft(segments, axis=-1)[:, :half]
        powers = (jnp.real(spectra) ** 2 + jnp.imag(spectra) ** 2) * norm_scale
        weights = keep_flags.astype(jnp.float32)
        peak_one = jnp.max(powers * weights[:, None], axis=0)
        log_one = jnp.sum(weights[:, None] * jnp.log(0.25 + powers), axis=0) / jnp.sum(weights)
        return peak_one, log_one

    peak_hold, log_mean = lax.map(one_channel, (hop_rows, gap_mask))
    onehot = (assignment[None, :] == jnp.arange(BLOCKS)[:, None]).astype(jnp.float32)
    block_sum = jnp.dot(onehot, log_mean, precision=lax.Precision.HIGHEST)
    block_mean = block_sum / jnp.sum(onehot, axis=1)[:, None]
    return peak_hold, log_mean, block_mean
```

```python
import functools
import math

import jax
import jax.numpy as jnp
import numpy as np
from jax import lax
from jax.experimental import pallas as pl
from jax.experimental.pallas import tpu as pltpu
from jax.sharding import PartitionSpec as P

LA = 256
LB = 128
BLOCKS = 8
MESH = pl.DeviceIdType.MESH
F32 = jnp.float32
BF16 = jnp.bfloat16


def split_constant(matrix):
    high = matrix.astype(BF16)
    low = (matrix - high.astype(np.float64)).astype(BF16)
    return high, low


def tables():
    length = LA * LB
    rows = LA // 2 + 8
    first = np.arange(rows)[:, None]
    used = first <= LA // 2
    angle = 2.0 * np.pi * (first * np.arange(LA)[None, :] % LA) / LA
    stage_one = np.concatenate([np.cos(angle) * used, -np.sin(angle) * used], axis=0)
    turn = 2.0 * np.pi * (first * np.arange(LB)[None, :]) / length
    twiddle = np.stack([np.cos(turn), -np.sin(turn)]).astype(np.float32)
    lane = np.arange(LB)
    second = np.where(lane < LB // 2, lane, LB - 1 - (lane - LB // 2))
    angle = 2.0 * np.pi * (np.arange(LB)[:, None] * second[None, :] % LB) / LB
    stage_two = np.block([[np.cos(angle), -np.sin(angle)], [np.sin(angle), np.cos(angle)]])
    samples = np.arange(length // 2)
    scale = 1.0 / math.sqrt(0.375 * length)
    rising = (0.5 - 0.5 * np.cos(samples * (2.0 * np.pi / length))) * scale
    falling = (0.5 + 0.5 * np.cos(samples * (2.0 * np.pi / length))) * scale
    window = np.stack([rising, falling]).reshape(2, LA // 2, LB).astype(np.float32)
    return (*split_constant(stage_one), *split_constant(stage_two), twiddle, window)


def split_value(x):
    high = x.astype(BF16)
    low = (x - high.astype(F32)).astype(BF16)
    return high, low


def three_pass(left, right):
    dot = functools.partial(jnp.dot, preferred_element_type=F32)
    return dot(left[0], right[0]) + dot(left[0], right[1]) + dot(left[1], right[0])


def kernel(
    sizes,
    assign_ref,
    x_ref,
    gap_ref,
    one_high,
    one_low,
    two_high,
    two_low,
    twiddle,
    window,
    peak_out,
    mean_out,
    block_out,
    work,
    away,
    stage,
    arrived,
    masks,
    sub_sums,
    chan_sums,
    peak_rows,
    mean_rows,
    raw_send,
    raw_recv,
    halo_send,
    halo_recv,
    mask_send,
    mask_recv,
    part_send,
    part_recv,
    sub_send,
    sub_recv,
    chan_send,
    chan_recv,
):
    times, subs, chans = sizes
    pairs = times // 2
    channels = x_ref.shape[0]
    nh = channels // 2
    rows = LA // 2
    out_rows = stage.shape[3]
    me = lax.axis_index("tm")
    pair, side = me // 2, lax.rem(me, 2)
    partner = pair * 2 + 1 - side
    my_sub = lax.axis_index("sub")
    my_chan = lax.axis_index("chan")

    barrier = pltpu.get_barrier_semaphore()
    for axis, here, count in (("tm", me, times), ("sub", my_sub, subs), ("chan", my_chan, chans)):
        for k in range(1, count):
            pl.semaphore_signal(
                barrier, inc=1, device_id={axis: lax.rem(here + k, count)}, device_id_type=MESH
            )

    for own in range(2):

        @pl.when(side == own)
        def _():
            for j in range(2 * rows):
                part = x_ref[:, j * LB : (j + 1) * LB]
                slot, row = j // rows, j % rows
                work[:, 2 * own + slot, row, :] = part[own * nh : (own + 1) * nh]
                away[:, slot, row, :] = part[(1 - own) * nh : (2 - own) * nh]

    flags = gap_ref[...].astype(F32)
    for s in range(2):
        masks[me, s] = jnp.broadcast_to(flags[:, s : s + 1], (channels, LB))

    @pl.when(pair == pairs - 1)
    def _():
        work[:, 4] = jnp.zeros_like(work[:, 4])

    pl.semaphore_wait(barrier, times + subs + chans - 3)

    def raw_copy(ci):
        return pltpu.make_async_remote_copy(
            src_ref=away.at[ci],
            dst_ref=work.at[ci, pl.ds(2 * side, 2)],
            send_sem=raw_send.at[ci],
            recv_sem=raw_recv.at[ci],
            device_id={"tm": partner},
            device_id_type=MESH,
        )

    def halo_copy(ci, which):
        return pltpu.make_async_remote_copy(
            src_ref=away.at[ci, 0] if which else work.at[ci, 0],
            dst_ref=work.at[ci, 4],
            send_sem=halo_send.at[which, ci],
            recv_sem=halo_recv.at[ci],
            device_id={"tm": jnp.maximum(2 * pair - 2 + which, 0)},
            device_id_type=MESH,
        )

    def mask_copy(k):
        return pltpu.make_async_remote_copy(
            src_ref=masks.at[me],
            dst_ref=masks.at[me],
            send_sem=mask_send.at[k],
            recv_sem=mask_recv.at[me],
            device_id={"tm": lax.rem(me + k, times)},
            device_id_type=MESH,
        )

    def part_copy(k, ci):
        target = lax.rem(me + k, times)
        return pltpu.make_async_remote_copy(
            src_ref=stage.at[target, ci],
            dst_ref=arrived.at[me, ci],
            send_sem=part_send.at[k, ci],
            recv_sem=part_recv.at[me, ci],
            device_id={"tm": target},
            device_id_type=MESH,
        )

    sends_halo = jnp.logical_and(side == 0, pair > 0)
    for k in range(1, times):
        mask_copy(k).start()
    for ci in range(nh):
        raw_copy(ci).start()

        @pl.when(sends_halo)
        def _():
            halo_copy(ci, 0).start()
            halo_copy(ci, 1).start()

    for k in range(1, times):
        source = lax.rem(me + k, times)
        pltpu.make_async_remote_copy(
            src_ref=masks.at[source],
            dst_ref=masks.at[source],
            send_sem=mask_send.at[k],
            recv_sem=mask_recv.at[source],
            device_id={"tm": source},
            device_id_type=MESH,
        ).wait_recv()

    lane = lax.broadcasted_iota(jnp.int32, (8, LB), 1)
    sub_row = lax.broadcasted_iota(jnp.int32, (8, LB), 0)
    swap = jnp.logical_and(sub_row == 0, lane >= LB // 2)
    mirror = lax.rem(LB - lax.broadcasted_iota(jnp.int32, (LB // 2, LB), 1), LB)

    def in_order(table):
        head = jnp.where(swap, jnp.broadcast_to(table[rows : rows + 1], (8, LB)), table[:8])
        turned = jnp.concatenate([head, table[8:rows]], axis=0).T
        back = jnp.take_along_axis(turned[LB // 2 :], mirror, axis=1)
        return jnp.concatenate([turned[: LB // 2], back], axis=1)

    def one_channel(ci, carry):
        raw_copy(ci).wait_recv()

        @pl.when(pair < pairs - 1)
        def _():
            halo_copy(ci, 0).wait_recv()

        columns_high, columns_low = [], []
        for s in range(4):
            frame = jnp.concatenate(
                [work[ci, s] * window[0], work[ci, s + 1] * window[1]], axis=0
            )
            high, low = split_value(frame)
            columns_high.append(high)
            columns_low.append(low)
        frames = (jnp.concatenate(columns_high, axis=1), jnp.concatenate(columns_low, axis=1))
        middle = three_pass((one_high[...], one_low[...]), frames)
        real, imag = middle[: rows + 8], middle[rows + 8 :]
        cosine, sine = twiddle[0], twiddle[1]
        turned = []
        for s in range(4):
            re, im = real[:, s * LB : (s + 1) * LB], imag[:, s * LB : (s + 1) * LB]
            turned.append(
                jnp.concatenate([re * cosine - im * sine, re * sine + im * cosine], axis=1)
            )
        turned = jnp.concatenate(turned, axis=0)
        bins = three_pass(split_value(turned), (two_high[...], two_low[...]))
        powers = bins[:, :LB] * bins[:, :LB] + bins[:, LB:] * bins[:, LB:]
        channel = side * nh + ci
        peak, product = None, None
        for s in range(4):
            keep = masks[2 * pair + s // 2, s % 2, pl.ds(channel, 1), :] > 0.5
            here = powers[s * (rows + 8) : (s + 1) * (rows + 8)]
            held = jnp.where(keep, here, 0.0)
            factor = jnp.where(keep, here + 0.25, 1.0)
            peak = held if peak is None else jnp.maximum(peak, held)
            product = factor if product is None else product * factor
        for which, table in enumerate((peak, jnp.log(product))):
            ordered = in_order(table)
            for target in range(times):
                stage[target, ci, which] = ordered[target * out_rows : (target + 1) * out_rows]
        for k in range(1, times):
            part_copy(k, ci).start()
        arrived[me, ci] = stage[me, ci]
        return carry

    lax.fori_loop(0, nh, one_channel, 0)

    kept = jnp.zeros((channels, LB), F32)
    for t in range(times):
        kept = kept + masks[t, 0] + masks[t, 1]

    for ci in range(nh):
        for k in range(1, times):
            source = lax.rem(me + k, times)
            pltpu.make_async_remote_copy(
                src_ref=arrived.at[source, ci],
                dst_ref=arrived.at[source, ci],
                send_sem=part_send.at[k, ci],
                recv_sem=part_recv.at[source, ci],
                device_id={"tm": source},
                device_id_type=MESH,
            ).wait_recv()

    count_lane = lax.broadcasted_iota(jnp.int32, (out_rows, 2 * LB), 1)
    counts = jnp.zeros((out_rows, 2 * LB), F32)
    blocks = [jnp.zeros((out_rows, 2 * LB), F32) for _ in range(BLOCKS)]
    for c in range(channels):
        origin, ci = c // nh, c % nh
        peak = arrived[origin, ci, 0]
        logs = arrived[origin, ci, 1]
        for p in range(1, pairs):
            peak = jnp.maximum(peak, arrived[2 * p + origin, ci, 0])
            logs = logs + arrived[2 * p + origin, ci, 1]
        row = kept[c : c + 1]
        mean = logs / jnp.concatenate([row, row], axis=1)
        peak_rows[c] = peak
        mean_rows[c] = mean
        group = assign_ref[c]
        counts = counts + (count_lane == group).astype(F32)
        for b in range(BLOCKS):
            blocks[b] = blocks[b] + mean * (group == b).astype(F32)
    for b in range(BLOCKS):
        sub_sums[my_sub, b] = blocks[b]
    sub_sums[my_sub, BLOCKS] = counts

    def exchange(axis, here, count, sums, send, recv):
        def copy(k, owner):
            return pltpu.make_async_remote_copy(
                src_ref=sums.at[owner],
                dst_ref=sums.at[owner],
                send_sem=send.at[k],
                recv_sem=recv.at[owner],
                device_id={axis: lax.rem(here + k, count)},
                device_id_type=MESH,
            )

        sends = [copy(k, here) for k in range(1, count)]
        for one in sends:
            one.start()
        return sends, [copy(k, lax.rem(here + k, count)) for k in range(1, count)]

    sub_out, sub_in = exchange("sub", my_sub, subs, sub_sums, sub_send, sub_recv)
    for j in range(out_rows):
        for side_lane in range(2):
            at = (2 * j + side_lane) * LB
            lanes = slice(side_lane * LB, (side_lane + 1) * LB)
            peak_out[:, at : at + LB] = peak_rows[:, j, lanes]
            mean_out[:, at : at + LB] = mean_rows[:, j, lanes]
    for one in sub_in:
        one.wait_recv()
    for b in range(BLOCKS + 1):
        total = sub_sums[0, b]
        for k in range(1, subs):
            total = total + sub_sums[k, b]
        chan_sums[my_chan, b] = total
    chan_out, chan_in = exchange("chan", my_chan, chans, chan_sums, chan_send, chan_recv)
    for one in chan_in:
        one.wait_recv()
    totals = []
    for b in range(BLOCKS + 1):
        total = chan_sums[0, b]
        for k in range(1, chans):
            total = total + chan_sums[k, b]
        totals.append(total)
    for b in range(BLOCKS):
        size = jnp.sum(jnp.where(count_lane == b, totals[BLOCKS], 0.0), axis=1, keepdims=True)
        peak_rows[b] = totals[b] / size
    for j in range(out_rows):
        for side_lane in range(2):
            at = (2 * j + side_lane) * LB
            lanes = slice(side_lane * LB, (side_lane + 1) * LB)
            block_out[:, at : at + LB] = peak_rows[:BLOCKS, j, lanes]

    for one in sub_out + chan_out:
        one.wait_send()
    for k in range(1, times):
        mask_copy(k).wait_send()
    for ci in range(nh):
        raw_copy(ci).wait_send()

        @pl.when(sends_halo)
        def _():
            halo_copy(ci, 0).wait_send()
            halo_copy(ci, 1).wait_send()

        for k in range(1, times):
            part_copy(k, ci).wait_send()


def on_device(sizes, signal, gap_mask, assignment):
    times, subs, chans = sizes
    channels, local_time = signal.shape
    nh = channels // 2
    rows = LA // 2
    width = LA * LB // 2 // times
    out_rows = width // (2 * LB)
    constants = [jnp.asarray(t) for t in tables()]
    vmem = pl.BlockSpec(memory_space=pltpu.VMEM)
    dma = pltpu.SemaphoreType.DMA
    return pl.pallas_call(
        functools.partial(kernel, sizes),
        out_shape=[
            jax.ShapeDtypeStruct((channels, width), F32),
            jax.ShapeDtypeStruct((channels, width), F32),
            jax.ShapeDtypeStruct((BLOCKS, width), F32),
        ],
        in_specs=[pl.BlockSpec(memory_space=pltpu.SMEM)] + [vmem] * 8,
        out_specs=[vmem] * 3,
        scratch_shapes=[
            pltpu.VMEM((nh, 5, rows, LB), F32),
            pltpu.VMEM((nh, 2, rows, LB), F32),
            pltpu.VMEM((times, nh, 2, out_rows, 2 * LB), F32),
            pltpu.VMEM((times, nh, 2, out_rows, 2 * LB), F32),
            pltpu.VMEM((times, 2, channels, LB), F32),
            pltpu.VMEM((subs, BLOCKS + 1, out_rows, 2 * LB), F32),
            pltpu.VMEM((chans, BLOCKS + 1, out_rows, 2 * LB), F32),
            pltpu.VMEM((max(channels, BLOCKS), out_rows, 2 * LB), F32),
            pltpu.VMEM((channels, out_rows, 2 * LB), F32),
            dma((nh,)),
            dma((nh,)),
            dma((2, nh)),
            dma((nh,)),
            dma((times,)),
            dma((times,)),
            dma((times, nh)),
            dma((times, nh)),
            dma((subs,)),
            dma((subs,)),
            dma((chans,)),
            dma((chans,)),
        ],
        compiler_params=pltpu.CompilerParams(collective_id=0, has_side_effects=True),
    )(assignment, signal, gap_mask, *constants)


def solution(mesh):
    sizes = (mesh.shape["tm"], mesh.shape["sub"], mesh.shape["chan"])
    in_specs = (
        P(("grp", "chan", "sub"), "tm"),
        P(("grp", "chan", "sub"), "tm"),
        P(("grp", "chan", "sub")),
    )
    out_specs = (P(("grp", "chan", "sub"), "tm"), P(("grp", "chan", "sub"), "tm"), P("grp", "tm"))
    return jax.shard_map(
        functools.partial(on_device, sizes),
        mesh=mesh,
        in_specs=in_specs,
        out_specs=out_specs,
        check_vma=False,
    )
```

```python
import functools
import math

import jax
import jax.numpy as jnp
import numpy as np
from jax import lax
from jax.experimental import pallas as pl
from jax.experimental.pallas import tpu as pltpu
from jax.sharding import PartitionSpec as P

LA = 256
LB = 128
BLOCKS = 8
MESH = pl.DeviceIdType.MESH
F32 = jnp.float32
BF16 = jnp.bfloat16


def split_constant(matrix):
    high = matrix.astype(BF16)
    low = (matrix - high.astype(np.float64)).astype(BF16)
    return high, low


def tables():
    length = LA * LB
    rows = LA // 2 + 8
    first = np.arange(rows)[:, None]
    used = first <= LA // 2
    angle = 2.0 * np.pi * (first * np.arange(LA)[None, :] % LA) / LA
    stage_one = np.concatenate([np.cos(angle) * used, -np.sin(angle) * used], axis=0)
    turn = 2.0 * np.pi * (first * np.arange(LB)[None, :]) / length
    twiddle = np.stack([np.cos(turn), -np.sin(turn)]).astype(np.float32)
    lane = np.arange(LB)
    second = np.where(lane < LB // 2, lane, LB - 1 - (lane - LB // 2))
    angle = 2.0 * np.pi * (np.arange(LB)[:, None] * second[None, :] % LB) / LB
    stage_two = np.block([[np.cos(angle), -np.sin(angle)], [np.sin(angle), np.cos(angle)]])
    samples = np.arange(length // 2)
    scale = 1.0 / math.sqrt(0.375 * length)
    rising = (0.5 - 0.5 * np.cos(samples * (2.0 * np.pi / length))) * scale
    falling = (0.5 + 0.5 * np.cos(samples * (2.0 * np.pi / length))) * scale
    window = np.stack([rising, falling]).reshape(2, LA // 2, LB).astype(np.float32)
    return (*split_constant(stage_one), *split_constant(stage_two), twiddle, window)


def split_value(x):
    high = x.astype(BF16)
    low = (x - high.astype(F32)).astype(BF16)
    return high, low


def three_pass(left, right):
    dot = functools.partial(jnp.dot, preferred_element_type=F32)
    return dot(left[0], right[0]) + dot(left[0], right[1]) + dot(left[1], right[0])


def kernel(
    sizes,
    assign_ref,
    x_ref,
    gap_ref,
    one_high,
    one_low,
    two_high,
    two_low,
    twiddle,
    window,
    peak_out,
    mean_out,
    block_out,
    work,
    away,
    stage,
    arrived,
    masks,
    sub_sums,
    chan_sums,
    peak_rows,
    mean_rows,
    raw_send,
    raw_recv,
    halo_send,
    halo_recv,
    mask_send,
    mask_recv,
    part_send,
    part_recv,
    sub_send,
    sub_recv,
    chan_send,
    chan_recv,
):
    times, subs, chans = sizes
    pairs = times // 2
    channels = x_ref.shape[0]
    nh = channels // 2
    rows = LA // 2
    out_rows = stage.shape[3]
    me = lax.axis_index("tm")
    pair, side = me // 2, lax.rem(me, 2)
    partner = pair * 2 + 1 - side
    my_sub = lax.axis_index("sub")
    my_chan = lax.axis_index("chan")

    barrier = pltpu.get_barrier_semaphore()
    for axis, here, count in (("tm", me, times), ("sub", my_sub, subs), ("chan", my_chan, chans)):
        for k in range(1, count):
            pl.semaphore_signal(
                barrier, inc=1, device_id={axis: lax.rem(here + k, count)}, device_id_type=MESH
            )

    for own in range(2):

        @pl.when(side == own)
        def _():
            for j in range(2 * rows):
                part = x_ref[:, j * LB : (j + 1) * LB]
                slot, row = j // rows, j % rows
                work[:, 1 + 2 * own + slot, row, :] = part[own * nh : (own + 1) * nh]
                away[:, slot, row, :] = part[(1 - own) * nh : (2 - own) * nh]

    channel_row = lax.broadcasted_iota(jnp.int32, (channels, LB), 0)
    for s in range(2):
        flags = jnp.zeros((channels, LB), F32)
        for c in range(channels):
            flags = jnp.where(channel_row == c, gap_ref[s, c].astype(F32), flags)
        masks[me, s] = flags

    across = me - 1 + 2 * side
    has_across = jnp.logical_and(across >= 0, across < times)

    for own in range(2):
        empty = 0 if own else 5

        @pl.when(side == own)
        def _():
            work[:, empty] = jnp.zeros_like(work[:, empty])

        @pl.when(jnp.logical_and(side == own, jnp.logical_not(has_across)))
        def _():
            work[:, 5 - empty] = jnp.zeros_like(work[:, 5 - empty])

    pl.semaphore_wait(barrier, times + subs + chans - 3)

    def raw_copy(ci):
        return pltpu.make_async_remote_copy(
            src_ref=away.at[ci],
            dst_ref=work.at[ci, pl.ds(1 + 2 * side, 2)],
            send_sem=raw_send.at[ci],
            recv_sem=raw_recv.at[ci],
            device_id={"tm": partner},
            device_id_type=MESH,
        )

    def halo_copy(ci):
        return pltpu.make_async_remote_copy(
            src_ref=away.at[ci, side],
            dst_ref=work.at[ci, 5 * (1 - side)],
            send_sem=halo_send.at[ci],
            recv_sem=halo_recv.at[ci],
            device_id={"tm": lax.clamp(0, across, times - 1)},
            device_id_type=MESH,
        )

    def mask_copy(k):
        return pltpu.make_async_remote_copy(
            src_ref=masks.at[me],
            dst_ref=masks.at[me],
            send_sem=mask_send.at[k],
            recv_sem=mask_recv.at[me],
            device_id={"tm": lax.rem(me + k, times)},
            device_id_type=MESH,
        )

    def part_copy(k, ci):
        target = lax.rem(me + k, times)
        return pltpu.make_async_remote_copy(
            src_ref=stage.at[target, ci],
            dst_ref=arrived.at[me, ci],
            send_sem=part_send.at[k, ci],
            recv_sem=part_recv.at[me, ci],
            device_id={"tm": target},
            device_id_type=MESH,
        )

    for k in range(1, times):
        mask_copy(k).start()
    for ci in range(nh):
        raw_copy(ci).start()

        @pl.when(has_across)
        def _():
            halo_copy(ci).start()

    for k in range(1, times):
        source = lax.rem(me + k, times)
        pltpu.make_async_remote_copy(
            src_ref=masks.at[source],
            dst_ref=masks.at[source],
            send_sem=mask_send.at[k],
            recv_sem=mask_recv.at[source],
            device_id={"tm": source},
            device_id_type=MESH,
        ).wait_recv()

    lane = lax.broadcasted_iota(jnp.int32, (8, LB), 1)
    sub_row = lax.broadcasted_iota(jnp.int32, (8, LB), 0)
    swap = jnp.logical_and(sub_row == 0, lane >= LB // 2)
    mirror = lax.rem(LB - lax.broadcasted_iota(jnp.int32, (LB // 2, LB), 1), LB)

    def in_order(table):
        head = jnp.where(swap, jnp.broadcast_to(table[rows : rows + 1], (8, LB)), table[:8])
        turned = jnp.concatenate([head, table[8:rows]], axis=0).T
        back = jnp.take_along_axis(turned[LB // 2 :], mirror, axis=1)
        return jnp.concatenate([turned[: LB // 2], back], axis=1)

    def one_channel(ci, carry):
        raw_copy(ci).wait_recv()

        @pl.when(has_across)
        def _():
            halo_copy(ci).wait_recv()

        columns_high, columns_low = [], []
        for s in range(5):
            frame = jnp.concatenate(
                [work[ci, s] * window[0], work[ci, s + 1] * window[1]], axis=0
            )
            high, low = split_value(frame)
            columns_high.append(high)
            columns_low.append(low)
        frames = (jnp.concatenate(columns_high, axis=1), jnp.concatenate(columns_low, axis=1))
        middle = three_pass((one_high[...], one_low[...]), frames)
        real, imag = middle[: rows + 8], middle[rows + 8 :]
        cosine, sine = twiddle[0], twiddle[1]
        turned = []
        for s in range(5):
            re, im = real[:, s * LB : (s + 1) * LB], imag[:, s * LB : (s + 1) * LB]
            turned.append(
                jnp.concatenate([re * cosine - im * sine, re * sine + im * cosine], axis=1)
            )
        turned = jnp.concatenate(turned, axis=0)
        bins = three_pass(split_value(turned), (two_high[...], two_low[...]))
        powers = bins[:, :LB] * bins[:, :LB] + bins[:, LB:] * bins[:, LB:]
        channel = side * nh + ci
        owned = [jnp.float32(1.0)] * 5
        owned[0] = jnp.logical_and(side == 0, has_across).astype(F32)
        owned[4] = jnp.logical_or(side == 1, pair == pairs - 1).astype(F32)
        peak, product = None, None
        for s in range(5):
            holder = jnp.maximum(2 * pair + (s - 1) // 2, 0)
            keep = masks[holder, (s - 1) % 2, pl.ds(channel, 1), :] * owned[s] > 0.5
            here = powers[s * (rows + 8) : (s + 1) * (rows + 8)]
            held = jnp.where(keep, here, 0.0)
            factor = jnp.where(keep, here + 0.25, 1.0)
            peak = held if peak is None else jnp.maximum(peak, held)
            product = factor if product is None else product * factor
        for which, table in enumerate((peak, jnp.log(product))):
            ordered = in_order(table)
            for target in range(times):
                stage[target, ci, which] = ordered[target * out_rows : (target + 1) * out_rows]
        for k in range(1, times):
            part_copy(k, ci).start()
        arrived[me, ci] = stage[me, ci]
        return carry

    lax.fori_loop(0, nh, one_channel, 0)

    kept = jnp.zeros((channels, LB), F32)
    for t in range(times):
        kept = kept + masks[t, 0] + masks[t, 1]

    count_lane = lax.broadcasted_iota(jnp.int32, (out_rows, 2 * LB), 1)
    counts = jnp.zeros((out_rows, 2 * LB), F32)
    blocks = [jnp.zeros((out_rows, 2 * LB), F32) for _ in range(BLOCKS)]
    for c in [half * nh + ci for ci in range(nh) for half in range(2)]:
        origin, ci = c // nh, c % nh
        if origin == 0:
            for k in range(1, times):
                source = lax.rem(me + k, times)
                pltpu.make_async_remote_copy(
                    src_ref=arrived.at[source, ci],
                    dst_ref=arrived.at[source, ci],
                    send_sem=part_send.at[k, ci],
                    recv_sem=part_recv.at[source, ci],
                    device_id={"tm": source},
                    device_id_type=MESH,
                ).wait_recv()
        peak = arrived[origin, ci, 0]
        logs = arrived[origin, ci, 1]
        for p in range(1, pairs):
            peak = jnp.maximum(peak, arrived[2 * p + origin, ci, 0])
            logs = logs + arrived[2 * p + origin, ci, 1]
        row = kept[c : c + 1]
        mean = logs / jnp.concatenate([row, row], axis=1)
        peak_rows[c] = peak
        mean_rows[c] = mean
        group = assign_ref[c]
        counts = counts + (count_lane == group).astype(F32)
        for b in range(BLOCKS):
            blocks[b] = blocks[b] + mean * (group == b).astype(F32)
    for b in range(BLOCKS):
        sub_sums[my_sub, b] = blocks[b]
    sub_sums[my_sub, BLOCKS] = counts

    def exchange(axis, here, count, sums, send, recv):
        def copy(k, owner):
            return pltpu.make_async_remote_copy(
                src_ref=sums.at[owner],
                dst_ref=sums.at[owner],
                send_sem=send.at[k],
                recv_sem=recv.at[owner],
                device_id={axis: lax.rem(here + k, count)},
                device_id_type=MESH,
            )

        sends = [copy(k, here) for k in range(1, count)]
        for one in sends:
            one.start()
        return sends, [copy(k, lax.rem(here + k, count)) for k in range(1, count)]

    sub_out, sub_in = exchange("sub", my_sub, subs, sub_sums, sub_send, sub_recv)
    for j in range(out_rows):
        for side_lane in range(2):
            at = (2 * j + side_lane) * LB
            lanes = slice(side_lane * LB, (side_lane + 1) * LB)
            peak_out[:, at : at + LB] = peak_rows[:, j, lanes]
            mean_out[:, at : at + LB] = mean_rows[:, j, lanes]
    for one in sub_in:
        one.wait_recv()
    for b in range(BLOCKS + 1):
        total = sub_sums[0, b]
        for k in range(1, subs):
            total = total + sub_sums[k, b]
        chan_sums[my_chan, b] = total
    chan_out, chan_in = exchange("chan", my_chan, chans, chan_sums, chan_send, chan_recv)
    for one in chan_in:
        one.wait_recv()
    totals = []
    for b in range(BLOCKS + 1):
        total = chan_sums[0, b]
        for k in range(1, chans):
            total = total + chan_sums[k, b]
        totals.append(total)
    for b in range(BLOCKS):
        size = jnp.sum(jnp.where(count_lane == b, totals[BLOCKS], 0.0), axis=1, keepdims=True)
        peak_rows[b] = totals[b] / size
    for j in range(out_rows):
        for side_lane in range(2):
            at = (2 * j + side_lane) * LB
            lanes = slice(side_lane * LB, (side_lane + 1) * LB)
            block_out[:, at : at + LB] = peak_rows[:BLOCKS, j, lanes]

    for one in sub_out + chan_out:
        one.wait_send()
    for k in range(1, times):
        mask_copy(k).wait_send()
    for ci in range(nh):
        raw_copy(ci).wait_send()

        @pl.when(has_across)
        def _():
            halo_copy(ci).wait_send()

        for k in range(1, times):
            part_copy(k, ci).wait_send()


def on_device(sizes, signal, gap_mask, assignment):
    times, subs, chans = sizes
    channels, local_time = signal.shape
    nh = channels // 2
    rows = LA // 2
    width = LA * LB // 2 // times
    out_rows = width // (2 * LB)
    constants = [jnp.asarray(t) for t in tables()]
    vmem = pl.BlockSpec(memory_space=pltpu.VMEM)
    smem = pl.BlockSpec(memory_space=pltpu.SMEM)
    dma = pltpu.SemaphoreType.DMA
    return pl.pallas_call(
        functools.partial(kernel, sizes),
        out_shape=[
            jax.ShapeDtypeStruct((channels, width), F32),
            jax.ShapeDtypeStruct((channels, width), F32),
            jax.ShapeDtypeStruct((BLOCKS, width), F32),
        ],
        in_specs=[smem, vmem, smem] + [vmem] * 6,
        out_specs=[vmem] * 3,
        scratch_shapes=[
            pltpu.VMEM((nh, 6, rows, LB), F32),
            pltpu.VMEM((nh, 2, rows, LB), F32),
            pltpu.VMEM((times, nh, 2, out_rows, 2 * LB), F32),
            pltpu.VMEM((times, nh, 2, out_rows, 2 * LB), F32),
            pltpu.VMEM((times, 2, channels, LB), F32),
            pltpu.VMEM((subs, BLOCKS + 1, out_rows, 2 * LB), F32),
            pltpu.VMEM((chans, BLOCKS + 1, out_rows, 2 * LB), F32),
            pltpu.VMEM((max(channels, BLOCKS), out_rows, 2 * LB), F32),
            pltpu.VMEM((channels, out_rows, 2 * LB), F32),
            dma((nh,)),
            dma((nh,)),
            dma((nh,)),
            dma((nh,)),
            dma((times,)),
            dma((times,)),
            dma((times, nh)),
            dma((times, nh)),
            dma((subs,)),
            dma((subs,)),
            dma((chans,)),
            dma((chans,)),
        ],
        compiler_params=pltpu.CompilerParams(collective_id=0, has_side_effects=True),
    )(assignment, signal, gap_mask.T, *constants)


def solution(mesh):
    sizes = (mesh.shape["tm"], mesh.shape["sub"], mesh.shape["chan"])
    in_specs = (
        P(("grp", "chan", "sub"), "tm"),
        P(("grp", "chan", "sub"), "tm"),
        P(("grp", "chan", "sub")),
    )
    out_specs = (P(("grp", "chan", "sub"), "tm"), P(("grp", "chan", "sub"), "tm"), P("grp", "tm"))
    return jax.shard_map(
        functools.partial(on_device, sizes),
        mesh=mesh,
        in_specs=in_specs,
        out_specs=out_specs,
        check_vma=False,
    )
```

```python
import functools
import math

import jax
import jax.numpy as jnp
import numpy as np
from jax import lax
from jax.experimental import pallas as pl
from jax.experimental.pallas import tpu as pltpu
from jax.sharding import PartitionSpec as P

LA = 256
LB = 128
BLOCKS = 8
MESH = pl.DeviceIdType.MESH
F32 = jnp.float32
BF16 = jnp.bfloat16


def split_constant(matrix):
    high = matrix.astype(BF16)
    low = (matrix - high.astype(np.float64)).astype(BF16)
    return high, low


def tables():
    length = LA * LB
    rows = LA // 2 + 8
    first = np.arange(rows)[:, None]
    used = first <= LA // 2
    angle = 2.0 * np.pi * (first * np.arange(LA)[None, :] % LA) / LA
    stage_one = np.concatenate([np.cos(angle) * used, -np.sin(angle) * used], axis=0)
    turn = 2.0 * np.pi * (first * np.arange(LB)[None, :]) / length
    twiddle = np.stack([np.cos(turn), -np.sin(turn)]).astype(np.float32)
    lane = np.arange(LB)
    second = np.where(lane < LB // 2, lane, LB - 1 - (lane - LB // 2))
    angle = 2.0 * np.pi * (np.arange(LB)[:, None] * second[None, :] % LB) / LB
    stage_two = np.block([[np.cos(angle), -np.sin(angle)], [np.sin(angle), np.cos(angle)]])
    samples = np.arange(length // 2)
    scale = 1.0 / math.sqrt(0.375 * length)
    rising = (0.5 - 0.5 * np.cos(samples * (2.0 * np.pi / length))) * scale
    falling = (0.5 + 0.5 * np.cos(samples * (2.0 * np.pi / length))) * scale
    window = np.stack([rising, falling]).reshape(2, LA // 2, LB).astype(np.float32)
    return (*split_constant(stage_one), *split_constant(stage_two), twiddle, window)


def split_value(x):
    high = x.astype(BF16)
    low = (x - high.astype(F32)).astype(BF16)
    return high, low


def three_pass(left, right):
    dot = functools.partial(jnp.dot, preferred_element_type=F32)
    return dot(left[0], right[0]) + dot(left[0], right[1]) + dot(left[1], right[0])


def kernel(
    sizes,
    assign_ref,
    x_in,
    gap_ref,
    *refs,
):
    inputs = (x_in, *refs[:6])
    peak_out, mean_out, block_out = refs[6:9]
    local = refs[9:16]
    x_ref, one_high, one_low, two_high, two_low, twiddle, window = local
    (
    work,
    away,
    stage,
    arrived,
    masks,
    means,
    owners,
    local_sem,
    raw_send,
    raw_recv,
    halo_send,
    halo_recv,
    mask_send,
    mask_recv,
    part_send,
    part_recv,
    mean_send,
    mean_recv,
    owner_send,
    owner_recv,
    ) = refs[16:]
    times, subs, chans = sizes
    pairs = times // 2
    channels = x_ref.shape[0]
    nh = channels // 2
    rows = LA // 2
    out_rows = stage.shape[3]
    peers = subs * chans
    me = lax.axis_index("tm")
    pair, side = me // 2, lax.rem(me, 2)
    partner = pair * 2 + 1 - side
    my_sub = lax.axis_index("sub")
    my_chan = lax.axis_index("chan")
    mine = my_chan * subs + my_sub
    copies = [pltpu.make_async_copy(a, b, local_sem.at[i]) for i, (a, b) in enumerate(zip(inputs, local))]
    for one in copies:
        one.start()

    def peer(k):
        other = lax.rem(mine + k, peers)
        return {"chan": other // subs, "sub": lax.rem(other, subs)}

    barrier = pltpu.get_barrier_semaphore()
    for k in range(1, times):
        pl.semaphore_signal(
            barrier, inc=1, device_id={"tm": lax.rem(me + k, times)}, device_id_type=MESH
        )
    for k in range(1, peers):
        pl.semaphore_signal(barrier, inc=1, device_id=peer(k), device_id_type=MESH)

    copies[0].wait()
    for own in range(2):

        @pl.when(side == own)
        def _():
            for j in range(2 * rows):
                part = x_ref[:, j * LB : (j + 1) * LB]
                slot, row = j // rows, j % rows
                work[:, 1 + 2 * own + slot, row, :] = part[own * nh : (own + 1) * nh]
                away[:, slot, row, :] = part[(1 - own) * nh : (2 - own) * nh]

    channel_row = lax.broadcasted_iota(jnp.int32, (channels, LB), 0)
    for s in range(2):
        flags = jnp.zeros((channels, LB), F32)
        for c in range(channels):
            flags = jnp.where(channel_row == c, gap_ref[s, c].astype(F32), flags)
        masks[me, s] = flags

    owner = jnp.zeros((channels, LB), jnp.int32)
    for c in range(channels):
        owner = jnp.where(channel_row == c, assign_ref[c], owner)
    owners[mine] = owner.astype(F32)

    across = me - 1 + 2 * side
    has_across = jnp.logical_and(across >= 0, across < times)

    for own in range(2):
        empty = 0 if own else 5

        @pl.when(side == own)
        def _():
            work[:, empty] = jnp.zeros_like(work[:, empty])

        @pl.when(jnp.logical_and(side == own, jnp.logical_not(has_across)))
        def _():
            work[:, 5 - empty] = jnp.zeros_like(work[:, 5 - empty])

    pl.semaphore_wait(barrier, times + peers - 2)

    def raw_copy(ci):
        return pltpu.make_async_remote_copy(
            src_ref=away.at[ci],
            dst_ref=work.at[ci, pl.ds(1 + 2 * side, 2)],
            send_sem=raw_send.at[ci],
            recv_sem=raw_recv.at[ci],
            device_id={"tm": partner},
            device_id_type=MESH,
        )

    def halo_copy(ci):
        return pltpu.make_async_remote_copy(
            src_ref=away.at[ci, side],
            dst_ref=work.at[ci, 5 * (1 - side)],
            send_sem=halo_send.at[ci],
            recv_sem=halo_recv.at[ci],
            device_id={"tm": lax.clamp(0, across, times - 1)},
            device_id_type=MESH,
        )

    def mask_copy(k):
        return pltpu.make_async_remote_copy(
            src_ref=masks.at[me],
            dst_ref=masks.at[me],
            send_sem=mask_send.at[k],
            recv_sem=mask_recv.at[me],
            device_id={"tm": lax.rem(me + k, times)},
            device_id_type=MESH,
        )

    def owner_copy(k, slot):
        return pltpu.make_async_remote_copy(
            src_ref=owners.at[slot],
            dst_ref=owners.at[slot],
            send_sem=owner_send.at[k],
            recv_sem=owner_recv.at[slot],
            device_id=peer(k),
            device_id_type=MESH,
        )

    def mean_copy(k, slot, ci):
        return pltpu.make_async_remote_copy(
            src_ref=means.at[slot, ci],
            dst_ref=means.at[slot, ci],
            send_sem=mean_send.at[k, ci],
            recv_sem=mean_recv.at[slot, ci],
            device_id=peer(k),
            device_id_type=MESH,
        )

    toward = jnp.where(2 * me < times, times - 1, 1)

    def part_copy(k, ci):
        target = lax.rem(me + k * toward, times)
        return pltpu.make_async_remote_copy(
            src_ref=stage.at[target, ci],
            dst_ref=arrived.at[me, ci],
            send_sem=part_send.at[k, ci],
            recv_sem=part_recv.at[me, ci],
            device_id={"tm": target},
            device_id_type=MESH,
        )

    for k in range(1, times):
        mask_copy(k).start()
    for k in range(1, peers):
        owner_copy(k, mine).start()
    for ci in range(nh):
        raw_copy(ci).start()

        @pl.when(has_across)
        def _():
            halo_copy(ci).start()

    for k in range(1, times):
        source = lax.rem(me + k, times)
        pltpu.make_async_remote_copy(
            src_ref=masks.at[source],
            dst_ref=masks.at[source],
            send_sem=mask_send.at[k],
            recv_sem=mask_recv.at[source],
            device_id={"tm": source},
            device_id_type=MESH,
        ).wait_recv()

    for k in range(1, peers):
        owner_copy(k, lax.rem(mine + k, peers)).wait_recv()
    for one in copies[1:]:
        one.wait()

    lane = lax.broadcasted_iota(jnp.int32, (8, LB), 1)
    sub_row = lax.broadcasted_iota(jnp.int32, (8, LB), 0)
    swap = jnp.logical_and(sub_row == 0, lane >= LB // 2)
    mirror = lax.rem(LB - lax.broadcasted_iota(jnp.int32, (LB // 2, LB), 1), LB)

    def in_order(table):
        head = jnp.where(swap, jnp.broadcast_to(table[rows : rows + 1], (8, LB)), table[:8])
        turned = jnp.concatenate([head, table[8:rows]], axis=0).T
        back = jnp.take_along_axis(turned[LB // 2 :], mirror, axis=1)
        return jnp.concatenate([turned[: LB // 2], back], axis=1)

    def one_channel(ci, carry):
        raw_copy(ci).wait_recv()

        @pl.when(has_across)
        def _():
            halo_copy(ci).wait_recv()

        columns_high, columns_low = [], []
        for s in range(5):
            frame = jnp.concatenate(
                [work[ci, s] * window[0], work[ci, s + 1] * window[1]], axis=0
            )
            high, low = split_value(frame)
            columns_high.append(high)
            columns_low.append(low)
        frames = (jnp.concatenate(columns_high, axis=1), jnp.concatenate(columns_low, axis=1))
        middle = three_pass((one_high[...], one_low[...]), frames)
        real, imag = middle[: rows + 8], middle[rows + 8 :]
        cosine, sine = twiddle[0], twiddle[1]
        turned = []
        for s in range(5):
            re, im = real[:, s * LB : (s + 1) * LB], imag[:, s * LB : (s + 1) * LB]
            turned.append(
                jnp.concatenate([re * cosine - im * sine, re * sine + im * cosine], axis=1)
            )
        turned = jnp.concatenate(turned, axis=0)
        bins = three_pass(split_value(turned), (two_high[...], two_low[...]))
        powers = bins[:, :LB] * bins[:, :LB] + bins[:, LB:] * bins[:, LB:]
        channel = side * nh + ci
        owned = [jnp.float32(1.0)] * 5
        owned[0] = jnp.logical_and(side == 0, has_across).astype(F32)
        owned[4] = jnp.logical_or(side == 1, pair == pairs - 1).astype(F32)
        peak, product = None, None
        for s in range(5):
            holder = jnp.maximum(2 * pair + (s - 1) // 2, 0)
            keep = masks[holder, (s - 1) % 2, pl.ds(channel, 1), :] * owned[s] > 0.5
            here = powers[s * (rows + 8) : (s + 1) * (rows + 8)]
            held = jnp.where(keep, here, 0.0)
            factor = jnp.where(keep, here + 0.25, 1.0)
            peak = held if peak is None else jnp.maximum(peak, held)
            product = factor if product is None else product * factor
        for which, table in enumerate((peak, jnp.log(product))):
            ordered = in_order(table)
            for target in range(times):
                stage[target, ci, which] = ordered[target * out_rows : (target + 1) * out_rows]
        for k in range(1, times):
            part_copy(k, ci).start()
        arrived[me, ci] = stage[me, ci]
        return carry

    lax.fori_loop(0, nh, one_channel, 0)

    kept = jnp.zeros((channels, LB), F32)
    for t in range(times):
        kept = kept + masks[t, 0] + masks[t, 1]

    blocks = [jnp.zeros((out_rows, 2 * LB), F32) for _ in range(BLOCKS)]

    def add_means(blocks, slot, ci):
        for half in range(2):
            mean = means[slot, ci, half]
            row = owners[slot, half * nh + ci : half * nh + ci + 1, :]
            row = jnp.concatenate([row, row], axis=1)
            blocks = [total + mean * (row == b).astype(F32) for b, total in enumerate(blocks)]
        return blocks

    for ci in range(nh):
        for k in range(1, times):
            source = lax.rem(me + k, times)
            pltpu.make_async_remote_copy(
                src_ref=arrived.at[source, ci],
                dst_ref=arrived.at[source, ci],
                send_sem=part_send.at[k, ci],
                recv_sem=part_recv.at[source, ci],
                device_id={"tm": source},
                device_id_type=MESH,
            ).wait_recv()
        for half in range(2):
            c = half * nh + ci
            peak = arrived[half, ci, 0]
            logs = arrived[half, ci, 1]
            for p in range(1, pairs):
                peak = jnp.maximum(peak, arrived[2 * p + half, ci, 0])
                logs = logs + arrived[2 * p + half, ci, 1]
            row = kept[c : c + 1]
            mean = logs / jnp.concatenate([row, row], axis=1)
            peak_out[c] = peak
            mean_out[c] = mean
            means[mine, ci, half] = mean
        for k in range(1, peers):
            mean_copy(k, mine, ci).start()
        if ci > 0:
            for k in range(1, peers):
                mean_copy(k, lax.rem(mine + k, peers), ci - 1).wait_recv()
            for slot in range(peers):
                blocks = add_means(blocks, slot, ci - 1)
    sizes_of = []
    for b in range(BLOCKS):
        held = jnp.zeros((channels, LB), F32)
        for slot in range(peers):
            held = held + (owners[slot] == b).astype(F32)
        size = jnp.sum(held, axis=0, keepdims=True)
        sizes_of.append(jnp.concatenate([size, size], axis=1))
    for k in range(1, peers):
        mean_copy(k, lax.rem(mine + k, peers), nh - 1).wait_recv()
    for slot in range(peers):
        blocks = add_means(blocks, slot, nh - 1)
    for b in range(BLOCKS):
        block_out[b] = blocks[b] / sizes_of[b]

    for k in range(1, peers):
        owner_copy(k, mine).wait_send()
        for ci in range(nh):
            mean_copy(k, mine, ci).wait_send()
    for k in range(1, times):
        mask_copy(k).wait_send()
    for ci in range(nh):
        raw_copy(ci).wait_send()

        @pl.when(has_across)
        def _():
            halo_copy(ci).wait_send()

        for k in range(1, times):
            part_copy(k, ci).wait_send()


def flatten(*refs):
    for lines, flat in zip(refs[:3], refs[3:]):
        for j in range(lines.shape[1]):
            for half in range(2):
                at = (2 * j + half) * LB
                flat[:, at : at + LB] = lines[:, j, half * LB : (half + 1) * LB]


def on_device(sizes, signal, gap_mask, assignment):
    times, subs, chans = sizes
    channels, local_time = signal.shape
    nh = channels // 2
    rows = LA // 2
    width = LA * LB // 2 // times
    out_rows = width // (2 * LB)
    peers = subs * chans
    constants = [jnp.asarray(t) for t in tables()]
    vmem = pl.BlockSpec(memory_space=pltpu.VMEM)
    smem = pl.BlockSpec(memory_space=pltpu.SMEM)
    hbm = pl.BlockSpec(memory_space=pl.ANY)
    dma = pltpu.SemaphoreType.DMA
    inputs = [signal, *constants]
    lines = [(channels, out_rows, 2 * LB)] * 2 + [(BLOCKS, out_rows, 2 * LB)]
    found = pl.pallas_call(
        functools.partial(kernel, sizes),
        out_shape=[jax.ShapeDtypeStruct(shape, F32) for shape in lines],
        in_specs=[smem, hbm, smem] + [hbm] * 6,
        out_specs=[vmem] * 3,
        scratch_shapes=[
            *[pltpu.VMEM(one.shape, one.dtype) for one in inputs],
            pltpu.VMEM((nh, 6, rows, LB), F32),
            pltpu.VMEM((nh, 2, rows, LB), F32),
            pltpu.VMEM((times, nh, 2, out_rows, 2 * LB), F32),
            pltpu.VMEM((times, nh, 2, out_rows, 2 * LB), F32),
            pltpu.VMEM((times, 2, channels, LB), F32),
            pltpu.VMEM((peers, nh, 2, out_rows, 2 * LB), F32),
            pltpu.VMEM((peers, channels, LB), F32),
            dma((len(inputs),)),
            dma((nh,)),
            dma((nh,)),
            dma((nh,)),
            dma((nh,)),
            dma((times,)),
            dma((times,)),
            dma((times, nh)),
            dma((times, nh)),
            dma((peers, nh)),
            dma((peers, nh)),
            dma((peers,)),
            dma((peers,)),
        ],
        compiler_params=pltpu.CompilerParams(collective_id=0, has_side_effects=True),
    )(assignment, signal, gap_mask.T, *constants)
    return pl.pallas_call(
        flatten,
        out_shape=[jax.ShapeDtypeStruct((shape[0], width), F32) for shape in lines],
        in_specs=[vmem] * 3,
        out_specs=[vmem] * 3,
    )(*found)


def solution(mesh):
    sizes = (mesh.shape["tm"], mesh.shape["sub"], mesh.shape["chan"])
    in_specs = (
        P(("grp", "chan", "sub"), "tm"),
        P(("grp", "chan", "sub"), "tm"),
        P(("grp", "chan", "sub")),
    )
    out_specs = (P(("grp", "chan", "sub"), "tm"), P(("grp", "chan", "sub"), "tm"), P("grp", "tm"))
    return jax.shard_map(
        functools.partial(on_device, sizes),
        mesh=mesh,
        in_specs=in_specs,
        out_specs=out_specs,
        check_vma=False,
    )
```

```python
import functools
import math

import jax
import jax.numpy as jnp
import numpy as np
from jax import lax
from jax.experimental import pallas as pl
from jax.experimental.pallas import tpu as pltpu
from jax.sharding import PartitionSpec as P

LA = 256
LB = 128
BLOCKS = 8
MESH = pl.DeviceIdType.MESH
F32 = jnp.float32
BF16 = jnp.bfloat16


def split_constant(matrix):
    high = matrix.astype(BF16)
    low = (matrix - high.astype(np.float64)).astype(BF16)
    return high, low


def tables():
    length = LA * LB
    rows = LA // 2 + 8
    first = np.arange(rows)[:, None]
    used = first <= LA // 2
    angle = 2.0 * np.pi * (first * np.arange(LA)[None, :] % LA) / LA
    stage_one = np.concatenate([np.cos(angle) * used, -np.sin(angle) * used], axis=0)
    turn = 2.0 * np.pi * (first * np.arange(LB)[None, :]) / length
    twiddle = np.stack([np.cos(turn), -np.sin(turn)]).astype(np.float32)
    lane = np.arange(LB)
    second = np.where(lane < LB // 2, lane, LB - 1 - (lane - LB // 2))
    angle = 2.0 * np.pi * (np.arange(LB)[:, None] * second[None, :] % LB) / LB
    stage_two = np.block([[np.cos(angle), -np.sin(angle)], [np.sin(angle), np.cos(angle)]])
    samples = np.arange(length // 2)
    scale = 1.0 / math.sqrt(0.375 * length)
    rising = (0.5 - 0.5 * np.cos(samples * (2.0 * np.pi / length))) * scale
    falling = (0.5 + 0.5 * np.cos(samples * (2.0 * np.pi / length))) * scale
    window = np.stack([rising, falling]).reshape(2, LA // 2, LB).astype(np.float32)
    return (*split_constant(stage_one), *split_constant(stage_two), twiddle, window)


def split_value(x):
    high = x.astype(BF16)
    low = (x - high.astype(F32)).astype(BF16)
    return high, low


def three_pass(left, right):
    dot = functools.partial(jnp.dot, preferred_element_type=F32)
    return dot(left[0], right[0]) + dot(left[0], right[1]) + dot(left[1], right[0])


def kernel(
    sizes,
    assign_ref,
    x_in,
    gap_ref,
    *refs,
):
    inputs = (x_in, *refs[:6])
    peak_out, mean_out, block_out = refs[6:9]
    local = refs[9:16]
    x_ref, one_high, one_low, two_high, two_low, twiddle, window = local
    (
    work,
    away,
    stage,
    arrived,
    masks,
    means,
    owners,
    local_sem,
    raw_send,
    raw_recv,
    halo_send,
    halo_recv,
    mask_send,
    mask_recv,
    part_send,
    part_recv,
    mean_send,
    mean_recv,
    owner_send,
    owner_recv,
    ) = refs[16:]
    times, subs, chans = sizes
    pairs = times // 2
    channels = x_ref.shape[0]
    nh = channels // 2
    rows = LA // 2
    out_rows = stage.shape[3]
    peers = subs * chans
    me = lax.axis_index("tm")
    pair, side = me // 2, lax.rem(me, 2)
    partner = pair * 2 + 1 - side
    my_sub = lax.axis_index("sub")
    my_chan = lax.axis_index("chan")
    mine = my_chan * subs + my_sub
    copies = [pltpu.make_async_copy(a, b, local_sem.at[i]) for i, (a, b) in enumerate(zip(inputs, local))]
    for one in copies:
        one.start()

    def peer(k):
        other = lax.rem(mine + k, peers)
        return {"chan": other // subs, "sub": lax.rem(other, subs)}

    barrier = pltpu.get_barrier_semaphore()
    for k in range(1, times):
        pl.semaphore_signal(
            barrier, inc=1, device_id={"tm": lax.rem(me + k, times)}, device_id_type=MESH
        )
    for k in range(1, peers):
        pl.semaphore_signal(barrier, inc=1, device_id=peer(k), device_id_type=MESH)

    copies[0].wait()
    for own in range(2):

        @pl.when(side == own)
        def _():
            for j in range(2 * rows):
                part = x_ref[:, j * LB : (j + 1) * LB]
                slot, row = j // rows, j % rows
                work[:, 1 + 2 * own + slot, row, :] = part[own * nh : (own + 1) * nh]
                away[:, slot, row, :] = part[(1 - own) * nh : (2 - own) * nh]

    channel_row = lax.broadcasted_iota(jnp.int32, (channels, LB), 0)
    for s in range(2):
        flags = jnp.zeros((channels, LB), F32)
        for c in range(channels):
            flags = jnp.where(channel_row == c, gap_ref[s, c].astype(F32), flags)
        masks[me, s] = flags

    owner = jnp.zeros((channels, LB), jnp.int32)
    for c in range(channels):
        owner = jnp.where(channel_row == c, assign_ref[c], owner)
    owners[mine] = owner.astype(F32)

    across = me - 1 + 2 * side
    has_across = jnp.logical_and(across >= 0, across < times)

    for own in range(2):
        empty = 0 if own else 5

        @pl.when(side == own)
        def _():
            work[:, empty] = jnp.zeros_like(work[:, empty])

        @pl.when(jnp.logical_and(side == own, jnp.logical_not(has_across)))
        def _():
            work[:, 5 - empty] = jnp.zeros_like(work[:, 5 - empty])

    pl.semaphore_wait(barrier, times + peers - 2)

    def raw_copy(ci):
        return pltpu.make_async_remote_copy(
            src_ref=away.at[ci],
            dst_ref=work.at[ci, pl.ds(1 + 2 * side, 2)],
            send_sem=raw_send.at[ci],
            recv_sem=raw_recv.at[ci],
            device_id={"tm": partner},
            device_id_type=MESH,
        )

    def halo_copy(ci):
        return pltpu.make_async_remote_copy(
            src_ref=away.at[ci, side],
            dst_ref=work.at[ci, 5 * (1 - side)],
            send_sem=halo_send.at[ci],
            recv_sem=halo_recv.at[ci],
            device_id={"tm": lax.clamp(0, across, times - 1)},
            device_id_type=MESH,
        )

    def mask_copy(k):
        return pltpu.make_async_remote_copy(
            src_ref=masks.at[me],
            dst_ref=masks.at[me],
            send_sem=mask_send.at[k],
            recv_sem=mask_recv.at[me],
            device_id={"tm": lax.rem(me + k, times)},
            device_id_type=MESH,
        )

    def owner_copy(k, slot):
        return pltpu.make_async_remote_copy(
            src_ref=owners.at[slot],
            dst_ref=owners.at[slot],
            send_sem=owner_send.at[k],
            recv_sem=owner_recv.at[slot],
            device_id=peer(k),
            device_id_type=MESH,
        )

    def mean_copy(k, slot, ci):
        return pltpu.make_async_remote_copy(
            src_ref=means.at[slot, ci],
            dst_ref=means.at[slot, ci],
            send_sem=mean_send.at[k, ci],
            recv_sem=mean_recv.at[slot, ci],
            device_id=peer(k),
            device_id_type=MESH,
        )

    toward = jnp.where(2 * me < times, times - 1, 1)

    def part_copy(k, ci, which):
        target = lax.rem(me + k * toward, times)
        return pltpu.make_async_remote_copy(
            src_ref=stage.at[target, ci, which],
            dst_ref=arrived.at[me, ci, which],
            send_sem=part_send.at[k, ci, which],
            recv_sem=part_recv.at[me, ci, which],
            device_id={"tm": target},
            device_id_type=MESH,
        )

    for k in range(1, times):
        mask_copy(k).start()
    for k in range(1, peers):
        owner_copy(k, mine).start()
    for ci in range(nh):
        raw_copy(ci).start()

        @pl.when(has_across)
        def _():
            halo_copy(ci).start()

    for k in range(1, times):
        source = lax.rem(me + k, times)
        pltpu.make_async_remote_copy(
            src_ref=masks.at[source],
            dst_ref=masks.at[source],
            send_sem=mask_send.at[k],
            recv_sem=mask_recv.at[source],
            device_id={"tm": source},
            device_id_type=MESH,
        ).wait_recv()

    for k in range(1, peers):
        owner_copy(k, lax.rem(mine + k, peers)).wait_recv()
    for one in copies[1:]:
        one.wait()

    lane = lax.broadcasted_iota(jnp.int32, (8, LB), 1)
    sub_row = lax.broadcasted_iota(jnp.int32, (8, LB), 0)
    swap = jnp.logical_and(sub_row == 0, lane >= LB // 2)
    mirror = lax.rem(LB - lax.broadcasted_iota(jnp.int32, (LB // 2, LB), 1), LB)

    def in_order(table):
        head = jnp.where(swap, jnp.broadcast_to(table[rows : rows + 1], (8, LB)), table[:8])
        turned = jnp.concatenate([head, table[8:rows]], axis=0).T
        back = jnp.take_along_axis(turned[LB // 2 :], mirror, axis=1)
        return jnp.concatenate([turned[: LB // 2], back], axis=1)

    def one_channel(ci, carry):
        raw_copy(ci).wait_recv()

        @pl.when(has_across)
        def _():
            halo_copy(ci).wait_recv()

        columns_high, columns_low = [], []
        for s in range(5):
            frame = jnp.concatenate(
                [work[ci, s] * window[0], work[ci, s + 1] * window[1]], axis=0
            )
            high, low = split_value(frame)
            columns_high.append(high)
            columns_low.append(low)
        frames = (jnp.concatenate(columns_high, axis=1), jnp.concatenate(columns_low, axis=1))
        middle = three_pass((one_high[...], one_low[...]), frames)
        real, imag = middle[: rows + 8], middle[rows + 8 :]
        cosine, sine = twiddle[0], twiddle[1]
        turned = []
        for s in range(5):
            re, im = real[:, s * LB : (s + 1) * LB], imag[:, s * LB : (s + 1) * LB]
            turned.append(
                jnp.concatenate([re * cosine - im * sine, re * sine + im * cosine], axis=1)
            )
        turned = jnp.concatenate(turned, axis=0)
        bins = three_pass(split_value(turned), (two_high[...], two_low[...]))
        powers = bins[:, :LB] * bins[:, :LB] + bins[:, LB:] * bins[:, LB:]
        channel = side * nh + ci
        owned = [jnp.float32(1.0)] * 5
        owned[0] = jnp.logical_and(side == 0, has_across).astype(F32)
        owned[4] = jnp.logical_or(side == 1, pair == pairs - 1).astype(F32)
        peak, product = None, None
        for s in range(5):
            holder = jnp.maximum(2 * pair + (s - 1) // 2, 0)
            keep = masks[holder, (s - 1) % 2, pl.ds(channel, 1), :] * owned[s] > 0.5
            here = powers[s * (rows + 8) : (s + 1) * (rows + 8)]
            held = jnp.where(keep, here, 0.0)
            factor = jnp.where(keep, here + 0.25, 1.0)
            peak = held if peak is None else jnp.maximum(peak, held)
            product = factor if product is None else product * factor
        for which, table in enumerate((peak, jnp.log(product))):
            ordered = in_order(table)
            for target in range(times):
                stage[target, ci, which] = ordered[target * out_rows : (target + 1) * out_rows]
        for k in range(1, times):
            part_copy(k, ci, 1).start()
        arrived[me, ci] = stage[me, ci]
        return carry

    lax.fori_loop(0, nh, one_channel, 0)
    for ci in range(nh):
        for k in range(1, times):
            part_copy(k, ci, 0).start()

    kept = jnp.zeros((channels, LB), F32)
    for t in range(times):
        kept = kept + masks[t, 0] + masks[t, 1]

    blocks = [jnp.zeros((out_rows, 2 * LB), F32) for _ in range(BLOCKS)]

    def add_means(blocks, slot, ci):
        for half in range(2):
            mean = means[slot, ci, half]
            row = owners[slot, half * nh + ci : half * nh + ci + 1, :]
            row = jnp.concatenate([row, row], axis=1)
            blocks = [total + mean * (row == b).astype(F32) for b, total in enumerate(blocks)]
        return blocks

    def await_parts(ci, which):
        for k in range(1, times):
            source = lax.rem(me + k, times)
            pltpu.make_async_remote_copy(
                src_ref=arrived.at[source, ci, which],
                dst_ref=arrived.at[source, ci, which],
                send_sem=part_send.at[k, ci, which],
                recv_sem=part_recv.at[source, ci, which],
                device_id={"tm": source},
                device_id_type=MESH,
            ).wait_recv()

    for ci in range(nh):
        await_parts(ci, 1)
        for half in range(2):
            c = half * nh + ci
            logs = arrived[half, ci, 1]
            for p in range(1, pairs):
                logs = logs + arrived[2 * p + half, ci, 1]
            row = kept[c : c + 1]
            mean = logs / jnp.concatenate([row, row], axis=1)
            mean_out[c] = mean
            means[mine, ci, half] = mean
        for k in range(1, peers):
            mean_copy(k, mine, ci).start()
        if ci > 0:
            for k in range(1, peers):
                mean_copy(k, lax.rem(mine + k, peers), ci - 1).wait_recv()
            for slot in range(peers):
                blocks = add_means(blocks, slot, ci - 1)
    for ci in range(nh):
        await_parts(ci, 0)
        for half in range(2):
            peak = arrived[half, ci, 0]
            for p in range(1, pairs):
                peak = jnp.maximum(peak, arrived[2 * p + half, ci, 0])
            peak_out[half * nh + ci] = peak
    sizes_of = []
    for b in range(BLOCKS):
        held = jnp.zeros((channels, LB), F32)
        for slot in range(peers):
            held = held + (owners[slot] == b).astype(F32)
        size = jnp.sum(held, axis=0, keepdims=True)
        sizes_of.append(jnp.concatenate([size, size], axis=1))
    for k in range(1, peers):
        mean_copy(k, lax.rem(mine + k, peers), nh - 1).wait_recv()
    for slot in range(peers):
        blocks = add_means(blocks, slot, nh - 1)
    for b in range(BLOCKS):
        block_out[b] = blocks[b] / sizes_of[b]

    for k in range(1, peers):
        owner_copy(k, mine).wait_send()
        for ci in range(nh):
            mean_copy(k, mine, ci).wait_send()
    for k in range(1, times):
        mask_copy(k).wait_send()
    for ci in range(nh):
        raw_copy(ci).wait_send()

        @pl.when(has_across)
        def _():
            halo_copy(ci).wait_send()

        for k in range(1, times):
            for which in range(2):
                part_copy(k, ci, which).wait_send()


def flatten(*refs):
    for lines, flat in zip(refs[:3], refs[3:]):
        for j in range(lines.shape[1]):
            for half in range(2):
                at = (2 * j + half) * LB
                flat[:, at : at + LB] = lines[:, j, half * LB : (half + 1) * LB]


def on_device(sizes, signal, gap_mask, assignment):
    times, subs, chans = sizes
    channels, local_time = signal.shape
    nh = channels // 2
    rows = LA // 2
    width = LA * LB // 2 // times
    out_rows = width // (2 * LB)
    peers = subs * chans
    constants = [jnp.asarray(t) for t in tables()]
    vmem = pl.BlockSpec(memory_space=pltpu.VMEM)
    smem = pl.BlockSpec(memory_space=pltpu.SMEM)
    hbm = pl.BlockSpec(memory_space=pl.ANY)
    dma = pltpu.SemaphoreType.DMA
    inputs = [signal, *constants]
    lines = [(channels, out_rows, 2 * LB)] * 2 + [(BLOCKS, out_rows, 2 * LB)]
    found = pl.pallas_call(
        functools.partial(kernel, sizes),
        out_shape=[jax.ShapeDtypeStruct(shape, F32) for shape in lines],
        in_specs=[smem, hbm, smem] + [hbm] * 6,
        out_specs=[vmem] * 3,
        scratch_shapes=[
            *[pltpu.VMEM(one.shape, one.dtype) for one in inputs],
            pltpu.VMEM((nh, 6, rows, LB), F32),
            pltpu.VMEM((nh, 2, rows, LB), F32),
            pltpu.VMEM((times, nh, 2, out_rows, 2 * LB), F32),
            pltpu.VMEM((times, nh, 2, out_rows, 2 * LB), F32),
            pltpu.VMEM((times, 2, channels, LB), F32),
            pltpu.VMEM((peers, nh, 2, out_rows, 2 * LB), F32),
            pltpu.VMEM((peers, channels, LB), F32),
            dma((len(inputs),)),
            dma((nh,)),
            dma((nh,)),
            dma((nh,)),
            dma((nh,)),
            dma((times,)),
            dma((times,)),
            dma((times, nh, 2)),
            dma((times, nh, 2)),
            dma((peers, nh)),
            dma((peers, nh)),
            dma((peers,)),
            dma((peers,)),
        ],
        compiler_params=pltpu.CompilerParams(collective_id=0, has_side_effects=True),
    )(assignment, signal, gap_mask.T, *constants)
    return pl.pallas_call(
        flatten,
        out_shape=[jax.ShapeDtypeStruct((shape[0], width), F32) for shape in lines],
        in_specs=[vmem] * 3,
        out_specs=[vmem] * 3,
    )(*found)


def solution(mesh):
    sizes = (mesh.shape["tm"], mesh.shape["sub"], mesh.shape["chan"])
    in_specs = (
        P(("grp", "chan", "sub"), "tm"),
        P(("grp", "chan", "sub"), "tm"),
        P(("grp", "chan", "sub")),
    )
    out_specs = (P(("grp", "chan", "sub"), "tm"), P(("grp", "chan", "sub"), "tm"), P("grp", "tm"))
    return jax.shard_map(
        functools.partial(on_device, sizes),
        mesh=mesh,
        in_specs=in_specs,
        out_specs=out_specs,
        check_vma=False,
    )
```

```python
import functools
import math

import jax
import jax.numpy as jnp
import numpy as np
from jax import lax
from jax.experimental import pallas as pl
from jax.experimental.pallas import tpu as pltpu
from jax.sharding import PartitionSpec as P

LA = 256
LB = 128
BLOCKS = 8
MESH = pl.DeviceIdType.MESH
F32 = jnp.float32
BF16 = jnp.bfloat16


def split_constant(matrix):
    high = matrix.astype(BF16)
    low = (matrix - high.astype(np.float64)).astype(BF16)
    return high, low


def tables():
    length = LA * LB
    rows = LA // 2 + 8
    first = np.arange(rows)[:, None]
    used = first <= LA // 2
    angle = 2.0 * np.pi * (first * np.arange(LA)[None, :] % LA) / LA
    stage_one = np.concatenate([np.cos(angle) * used, -np.sin(angle) * used], axis=0)
    turn = 2.0 * np.pi * (first * np.arange(LB)[None, :]) / length
    twiddle = np.stack([np.cos(turn), -np.sin(turn)]).astype(np.float32)
    lane = np.arange(LB)
    second = np.where(lane < LB // 2, lane, LB - 1 - (lane - LB // 2))
    angle = 2.0 * np.pi * (np.arange(LB)[:, None] * second[None, :] % LB) / LB
    stage_two = np.block([[np.cos(angle), -np.sin(angle)], [np.sin(angle), np.cos(angle)]])
    samples = np.arange(length // 2)
    scale = 1.0 / math.sqrt(0.375 * length)
    rising = (0.5 - 0.5 * np.cos(samples * (2.0 * np.pi / length))) * scale
    falling = (0.5 + 0.5 * np.cos(samples * (2.0 * np.pi / length))) * scale
    window = np.stack([rising, falling]).reshape(2, LA // 2, LB).astype(np.float32)
    return (*split_constant(stage_one), *split_constant(stage_two), twiddle, window)


def split_value(x):
    high = x.astype(BF16)
    low = (x - high.astype(F32)).astype(BF16)
    return high, low


def three_pass(left, right):
    dot = functools.partial(jnp.dot, preferred_element_type=F32)
    return dot(left[0], right[0]) + dot(left[0], right[1]) + dot(left[1], right[0])


def kernel(
    sizes,
    assign_ref,
    x_in,
    gap_ref,
    *refs,
):
    inputs = (x_in, *refs[:6])
    peak_out, mean_out, block_out = refs[6:9]
    local = refs[9:16]
    x_ref, one_high, one_low, two_high, two_low, twiddle, window = local
    (
    work,
    away,
    stage,
    arrived,
    masks,
    means,
    owners,
    local_sem,
    raw_send,
    raw_recv,
    halo_send,
    halo_recv,
    mask_send,
    mask_recv,
    part_send,
    part_recv,
    mean_send,
    mean_recv,
    owner_send,
    owner_recv,
    ) = refs[16:]
    times, subs, chans = sizes
    pairs = times // 2
    channels = x_ref.shape[0]
    nh = channels // 2
    rows = LA // 2
    out_rows = stage.shape[3]
    peers = subs * chans
    me = lax.axis_index("tm")
    pair, side = me // 2, lax.rem(me, 2)
    partner = pair * 2 + 1 - side
    my_sub = lax.axis_index("sub")
    my_chan = lax.axis_index("chan")
    mine = my_chan * subs + my_sub
    copies = [pltpu.make_async_copy(a, b, local_sem.at[i]) for i, (a, b) in enumerate(zip(inputs, local))]
    for one in copies:
        one.start()

    def peer(k):
        other = lax.rem(mine + k, peers)
        return {"chan": other // subs, "sub": lax.rem(other, subs)}

    barrier = pltpu.get_barrier_semaphore()
    for k in range(1, times):
        pl.semaphore_signal(
            barrier, inc=1, device_id={"tm": lax.rem(me + k, times)}, device_id_type=MESH
        )
    for k in range(1, peers):
        pl.semaphore_signal(barrier, inc=1, device_id=peer(k), device_id_type=MESH)

    copies[0].wait()
    for own in range(2):

        @pl.when(side == own)
        def _():
            for j in range(2 * rows):
                part = x_ref[:, j * LB : (j + 1) * LB]
                slot, row = j // rows, j % rows
                work[:, 1 + 2 * own + slot, row, :] = part[own * nh : (own + 1) * nh]
                away[:, slot, row, :] = part[(1 - own) * nh : (2 - own) * nh]

    channel_row = lax.broadcasted_iota(jnp.int32, (channels, LB), 0)
    for s in range(2):
        flags = jnp.zeros((channels, LB), F32)
        for c in range(channels):
            flags = jnp.where(channel_row == c, gap_ref[s, c].astype(F32), flags)
        masks[me, s] = flags

    owner = jnp.zeros((channels, LB), jnp.int32)
    for c in range(channels):
        owner = jnp.where(channel_row == c, assign_ref[c], owner)
    owners[mine] = owner.astype(F32)

    across = me - 1 + 2 * side
    has_across = jnp.logical_and(across >= 0, across < times)

    for own in range(2):
        empty = 0 if own else 5

        @pl.when(side == own)
        def _():
            work[:, empty] = jnp.zeros_like(work[:, empty])

        @pl.when(jnp.logical_and(side == own, jnp.logical_not(has_across)))
        def _():
            work[:, 5 - empty] = jnp.zeros_like(work[:, 5 - empty])

    pl.semaphore_wait(barrier, times + peers - 2)

    def raw_copy(ci):
        return pltpu.make_async_remote_copy(
            src_ref=away.at[ci],
            dst_ref=work.at[ci, pl.ds(1 + 2 * side, 2)],
            send_sem=raw_send.at[ci],
            recv_sem=raw_recv.at[ci],
            device_id={"tm": partner},
            device_id_type=MESH,
        )

    def halo_copy(ci):
        return pltpu.make_async_remote_copy(
            src_ref=away.at[ci, side],
            dst_ref=work.at[ci, 5 * (1 - side)],
            send_sem=halo_send.at[ci],
            recv_sem=halo_recv.at[ci],
            device_id={"tm": lax.clamp(0, across, times - 1)},
            device_id_type=MESH,
        )

    def mask_copy(k):
        return pltpu.make_async_remote_copy(
            src_ref=masks.at[me],
            dst_ref=masks.at[me],
            send_sem=mask_send.at[k],
            recv_sem=mask_recv.at[me],
            device_id={"tm": lax.rem(me + k, times)},
            device_id_type=MESH,
        )

    def owner_copy(k, slot):
        return pltpu.make_async_remote_copy(
            src_ref=owners.at[slot],
            dst_ref=owners.at[slot],
            send_sem=owner_send.at[k],
            recv_sem=owner_recv.at[slot],
            device_id=peer(k),
            device_id_type=MESH,
        )

    def mean_copy(k, slot, ci):
        return pltpu.make_async_remote_copy(
            src_ref=means.at[slot, ci],
            dst_ref=means.at[slot, ci],
            send_sem=mean_send.at[k, ci],
            recv_sem=mean_recv.at[slot, ci],
            device_id=peer(k),
            device_id_type=MESH,
        )

    toward = jnp.where(2 * me < times, times - 1, 1)

    def part_copy(k, ci, which):
        target = lax.rem(me + k * toward, times)
        return pltpu.make_async_remote_copy(
            src_ref=stage.at[target, ci, which],
            dst_ref=arrived.at[me, ci, which],
            send_sem=part_send.at[k, ci, which],
            recv_sem=part_recv.at[me, ci, which],
            device_id={"tm": target},
            device_id_type=MESH,
        )

    for k in range(1, times):
        mask_copy(k).start()
    for k in range(1, peers):
        owner_copy(k, mine).start()
    for ci in range(nh):
        raw_copy(ci).start()

        @pl.when(has_across)
        def _():
            halo_copy(ci).start()

    for k in range(1, times):
        source = lax.rem(me + k, times)
        pltpu.make_async_remote_copy(
            src_ref=masks.at[source],
            dst_ref=masks.at[source],
            send_sem=mask_send.at[k],
            recv_sem=mask_recv.at[source],
            device_id={"tm": source},
            device_id_type=MESH,
        ).wait_recv()

    for k in range(1, peers):
        owner_copy(k, lax.rem(mine + k, peers)).wait_recv()
    for one in copies[1:]:
        one.wait()

    lane = lax.broadcasted_iota(jnp.int32, (8, LB), 1)
    sub_row = lax.broadcasted_iota(jnp.int32, (8, LB), 0)
    swap = jnp.logical_and(sub_row == 0, lane >= LB // 2)
    mirror = lax.rem(LB - lax.broadcasted_iota(jnp.int32, (LB // 2, LB), 1), LB)

    def in_order(table):
        head = jnp.where(swap, jnp.broadcast_to(table[rows : rows + 1], (8, LB)), table[:8])
        turned = jnp.concatenate([head, table[8:rows]], axis=0).T
        back = jnp.take_along_axis(turned[LB // 2 :], mirror, axis=1)
        return jnp.concatenate([turned[: LB // 2], back], axis=1)

    def one_channel(ci, carry):
        raw_copy(ci).wait_recv()

        @pl.when(has_across)
        def _():
            halo_copy(ci).wait_recv()

        columns_high, columns_low = [], []
        for s in range(5):
            frame = jnp.concatenate(
                [work[ci, s] * window[0], work[ci, s + 1] * window[1]], axis=0
            )
            high, low = split_value(frame)
            columns_high.append(high)
            columns_low.append(low)
        frames = (jnp.concatenate(columns_high, axis=1), jnp.concatenate(columns_low, axis=1))
        middle = three_pass((one_high[...], one_low[...]), frames)
        real, imag = middle[: rows + 8], middle[rows + 8 :]
        cosine, sine = twiddle[0], twiddle[1]
        turned = []
        for s in range(5):
            re, im = real[:, s * LB : (s + 1) * LB], imag[:, s * LB : (s + 1) * LB]
            turned.append(
                jnp.concatenate([re * cosine - im * sine, re * sine + im * cosine], axis=1)
            )
        turned = jnp.concatenate(turned, axis=0)
        bins = three_pass(split_value(turned), (two_high[...], two_low[...]))
        powers = bins[:, :LB] * bins[:, :LB] + bins[:, LB:] * bins[:, LB:]
        channel = side * nh + ci
        owned = [jnp.float32(1.0)] * 5
        owned[0] = jnp.logical_and(side == 0, has_across).astype(F32)
        owned[4] = jnp.logical_or(side == 1, pair == pairs - 1).astype(F32)
        peak, product = None, None
        for s in range(5):
            holder = jnp.maximum(2 * pair + (s - 1) // 2, 0)
            keep = masks[holder, (s - 1) % 2, pl.ds(channel, 1), :] * owned[s] > 0.5
            here = powers[s * (rows + 8) : (s + 1) * (rows + 8)]
            held = jnp.where(keep, here, 0.0)
            factor = jnp.where(keep, here + 0.25, 1.0)
            peak = held if peak is None else jnp.maximum(peak, held)
            product = factor if product is None else product * factor
        for which, table in enumerate((peak, jnp.log(product))):
            ordered = in_order(table)
            for target in range(times):
                stage[target, ci, which] = ordered[target * out_rows : (target + 1) * out_rows]
        for k in range(1, times):
            part_copy(k, ci, 1).start()
        arrived[me, ci] = stage[me, ci]
        return carry

    lax.fori_loop(0, nh, one_channel, 0)
    for ci in range(nh):
        for k in range(1, times):
            part_copy(k, ci, 0).start()

    kept = jnp.zeros((channels, LB), F32)
    for t in range(times):
        kept = kept + masks[t, 0] + masks[t, 1]

    blocks = [jnp.zeros((out_rows, 2 * LB), F32) for _ in range(BLOCKS)]

    def add_means(blocks, slot, ci):
        for half in range(2):
            mean = means[slot, ci, half]
            row = owners[slot, half * nh + ci : half * nh + ci + 1, :]
            row = jnp.concatenate([row, row], axis=1)
            blocks = [total + mean * (row == b).astype(F32) for b, total in enumerate(blocks)]
        return blocks

    def await_parts(ci, which):
        for k in range(1, times):
            source = lax.rem(me + k, times)
            pltpu.make_async_remote_copy(
                src_ref=arrived.at[source, ci, which],
                dst_ref=arrived.at[source, ci, which],
                send_sem=part_send.at[k, ci, which],
                recv_sem=part_recv.at[source, ci, which],
                device_id={"tm": source},
                device_id_type=MESH,
            ).wait_recv()

    for ci in range(nh):
        await_parts(ci, 1)
        for half in range(2):
            c = half * nh + ci
            logs = arrived[half, ci, 1]
            for p in range(1, pairs):
                logs = logs + arrived[2 * p + half, ci, 1]
            row = kept[c : c + 1]
            mean = logs / jnp.concatenate([row, row], axis=1)
            mean_out[c] = mean
            means[mine, ci, half] = mean
        for k in range(1, peers):
            mean_copy(k, mine, ci).start()
        if ci > 0:
            for k in range(1, peers):
                mean_copy(k, lax.rem(mine + k, peers), ci - 1).wait_recv()
            for slot in range(peers):
                blocks = add_means(blocks, slot, ci - 1)
    for ci in range(nh):
        await_parts(ci, 0)
        for half in range(2):
            peak = arrived[half, ci, 0]
            for p in range(1, pairs):
                peak = jnp.maximum(peak, arrived[2 * p + half, ci, 0])
            peak_out[half * nh + ci] = peak
    sizes_of = []
    for b in range(BLOCKS):
        held = jnp.zeros((channels, LB), F32)
        for slot in range(peers):
            held = held + (owners[slot] == b).astype(F32)
        size = jnp.sum(held, axis=0, keepdims=True)
        sizes_of.append(jnp.concatenate([size, size], axis=1))
    for k in range(1, peers):
        mean_copy(k, lax.rem(mine + k, peers), nh - 1).wait_recv()
    for slot in range(peers):
        blocks = add_means(blocks, slot, nh - 1)
    for b in range(BLOCKS):
        block_out[b] = blocks[b] / sizes_of[b]

    for k in range(1, peers):
        owner_copy(k, mine).wait_send()
        for ci in range(nh):
            mean_copy(k, mine, ci).wait_send()
    for k in range(1, times):
        mask_copy(k).wait_send()
    for ci in range(nh):
        raw_copy(ci).wait_send()

        @pl.when(has_across)
        def _():
            halo_copy(ci).wait_send()

        for k in range(1, times):
            for which in range(2):
                part_copy(k, ci, which).wait_send()


def flatten(*refs):
    for lines, flat in zip(refs[:3], refs[3:]):
        for j in range(lines.shape[1]):
            for half in range(2):
                at = (2 * j + half) * LB
                flat[:, at : at + LB] = lines[:, j, half * LB : (half + 1) * LB]


def on_device(sizes, signal, gap_mask, assignment):
    times, subs, chans = sizes
    channels, local_time = signal.shape
    nh = channels // 2
    rows = LA // 2
    width = LA * LB // 2 // times
    out_rows = width // (2 * LB)
    peers = subs * chans
    constants = [jnp.asarray(t) for t in tables()]
    vmem = pl.BlockSpec(memory_space=pltpu.VMEM)
    smem = pl.BlockSpec(memory_space=pltpu.SMEM)
    hbm = pl.BlockSpec(memory_space=pl.ANY)
    dma = pltpu.SemaphoreType.DMA
    inputs = [signal, *constants]
    lines = [(channels, out_rows, 2 * LB)] * 2 + [(BLOCKS, out_rows, 2 * LB)]
    found = pl.pallas_call(
        functools.partial(kernel, sizes),
        out_shape=[pltpu.VMEM(shape, F32) for shape in lines],
        in_specs=[smem, hbm, smem] + [hbm] * 6,
        out_specs=[vmem] * 3,
        scratch_shapes=[
            *[pltpu.VMEM(one.shape, one.dtype) for one in inputs],
            pltpu.VMEM((nh, 6, rows, LB), F32),
            pltpu.VMEM((nh, 2, rows, LB), F32),
            pltpu.VMEM((times, nh, 2, out_rows, 2 * LB), F32),
            pltpu.VMEM((times, nh, 2, out_rows, 2 * LB), F32),
            pltpu.VMEM((times, 2, channels, LB), F32),
            pltpu.VMEM((peers, nh, 2, out_rows, 2 * LB), F32),
            pltpu.VMEM((peers, channels, LB), F32),
            dma((len(inputs),)),
            dma((nh,)),
            dma((nh,)),
            dma((nh,)),
            dma((nh,)),
            dma((times,)),
            dma((times,)),
            dma((times, nh, 2)),
            dma((times, nh, 2)),
            dma((peers, nh)),
            dma((peers, nh)),
            dma((peers,)),
            dma((peers,)),
        ],
        compiler_params=pltpu.CompilerParams(collective_id=0, has_side_effects=True),
    )(assignment, signal, gap_mask.T, *constants)
    return pl.pallas_call(
        flatten,
        out_shape=[jax.ShapeDtypeStruct((shape[0], width), F32) for shape in lines],
        in_specs=[vmem] * 3,
        out_specs=[vmem] * 3,
    )(*[pltpu.with_memory_space_constraint(one, pltpu.VMEM) for one in found])


def solution(mesh):
    sizes = (mesh.shape["tm"], mesh.shape["sub"], mesh.shape["chan"])
    in_specs = (
        P(("grp", "chan", "sub"), "tm"),
        P(("grp", "chan", "sub"), "tm"),
        P(("grp", "chan", "sub")),
    )
    out_specs = (P(("grp", "chan", "sub"), "tm"), P(("grp", "chan", "sub"), "tm"), P("grp", "tm"))
    return jax.shard_map(
        functools.partial(on_device, sizes),
        mesh=mesh,
        in_specs=in_specs,
        out_specs=out_specs,
        check_vma=False,
    )
```

```python
import functools
import math

import jax
import jax.numpy as jnp
import numpy as np
from jax import lax
from jax.experimental import pallas as pl
from jax.experimental.pallas import tpu as pltpu
from jax.sharding import PartitionSpec as P

LA = 256
LB = 128
BLOCKS = 8
MESH = pl.DeviceIdType.MESH
F32 = jnp.float32
BF16 = jnp.bfloat16


def split_constant(matrix):
    high = matrix.astype(BF16)
    low = (matrix - high.astype(np.float64)).astype(BF16)
    return high, low


def tables():
    length = LA * LB
    rows = LA // 2 + 8
    first = np.arange(rows)[:, None]
    used = first <= LA // 2
    angle = 2.0 * np.pi * (first * np.arange(LA)[None, :] % LA) / LA
    stage_one = np.concatenate([np.cos(angle) * used, -np.sin(angle) * used], axis=0)
    turn = 2.0 * np.pi * (first * np.arange(LB)[None, :]) / length
    twiddle = np.stack([np.cos(turn), -np.sin(turn)]).astype(np.float32)
    lane = np.arange(LB)
    second = np.where(lane < LB // 2, lane, LB - 1 - (lane - LB // 2))
    angle = 2.0 * np.pi * (np.arange(LB)[:, None] * second[None, :] % LB) / LB
    stage_two = np.block([[np.cos(angle), -np.sin(angle)], [np.sin(angle), np.cos(angle)]])
    samples = np.arange(length // 2)
    scale = 1.0 / math.sqrt(0.375 * length)
    rising = (0.5 - 0.5 * np.cos(samples * (2.0 * np.pi / length))) * scale
    falling = (0.5 + 0.5 * np.cos(samples * (2.0 * np.pi / length))) * scale
    window = np.stack([rising, falling]).reshape(2, LA // 2, LB).astype(np.float32)
    return (*split_constant(stage_one), *split_constant(stage_two), twiddle, window)


def split_value(x):
    high = x.astype(BF16)
    low = (x - high.astype(F32)).astype(BF16)
    return high, low


def three_pass(left, right):
    dot = functools.partial(jnp.dot, preferred_element_type=F32)
    return dot(left[0], right[0]) + dot(left[0], right[1]) + dot(left[1], right[0])


def kernel(
    sizes,
    assign_ref,
    x_in,
    gap_ref,
    *refs,
):
    inputs = (x_in, *refs[:6])
    peak_out, mean_out, block_out = refs[6:9]
    local = refs[9:16]
    x_ref, one_high, one_low, two_high, two_low, twiddle, window = local
    (
    work,
    away,
    stage,
    arrived,
    masks,
    means,
    owners,
    local_sem,
    raw_send,
    raw_recv,
    halo_send,
    halo_recv,
    mask_send,
    mask_recv,
    part_send,
    part_recv,
    mean_send,
    mean_recv,
    owner_send,
    owner_recv,
    ) = refs[16:]
    times, subs, chans = sizes
    pairs = times // 2
    channels = x_ref.shape[0]
    nh = channels // 2
    rows = LA // 2
    out_rows = stage.shape[3]
    peers = subs * chans
    me = lax.axis_index("tm")
    pair, side = me // 2, lax.rem(me, 2)
    partner = pair * 2 + 1 - side
    my_sub = lax.axis_index("sub")
    my_chan = lax.axis_index("chan")
    mine = my_chan * subs + my_sub
    copies = [pltpu.make_async_copy(a, b, local_sem.at[i]) for i, (a, b) in enumerate(zip(inputs, local))]
    for one in copies:
        one.start()

    def peer(k):
        other = lax.rem(mine + k, peers)
        return {"chan": other // subs, "sub": lax.rem(other, subs)}

    barrier = pltpu.get_barrier_semaphore()
    for k in range(1, times):
        pl.semaphore_signal(
            barrier, inc=1, device_id={"tm": lax.rem(me + k, times)}, device_id_type=MESH
        )
    for k in range(1, peers):
        pl.semaphore_signal(barrier, inc=1, device_id=peer(k), device_id_type=MESH)

    copies[0].wait()
    for own in range(2):

        @pl.when(side == own)
        def _():
            for j in range(2 * rows):
                part = x_ref[:, j * LB : (j + 1) * LB]
                slot, row = j // rows, j % rows
                work[:, 1 + 2 * own + slot, row, :] = part[own * nh : (own + 1) * nh]
                away[:, slot, row, :] = part[(1 - own) * nh : (2 - own) * nh]

    channel_row = lax.broadcasted_iota(jnp.int32, (channels, LB), 0)
    for s in range(2):
        flags = jnp.zeros((channels, LB), F32)
        for c in range(channels):
            flags = jnp.where(channel_row == c, gap_ref[s, c].astype(F32), flags)
        masks[me, s] = flags

    owner = jnp.zeros((channels, LB), jnp.int32)
    for c in range(channels):
        owner = jnp.where(channel_row == c, assign_ref[c], owner)
    owners[mine] = owner.astype(F32)

    across = me - 1 + 2 * side
    has_across = jnp.logical_and(across >= 0, across < times)

    for own in range(2):
        empty = 0 if own else 5

        @pl.when(side == own)
        def _():
            work[:, empty] = jnp.zeros_like(work[:, empty])

        @pl.when(jnp.logical_and(side == own, jnp.logical_not(has_across)))
        def _():
            work[:, 5 - empty] = jnp.zeros_like(work[:, 5 - empty])

    pl.semaphore_wait(barrier, times + peers - 2)

    def raw_copy(ci):
        return pltpu.make_async_remote_copy(
            src_ref=away.at[ci],
            dst_ref=work.at[ci, pl.ds(1 + 2 * side, 2)],
            send_sem=raw_send.at[ci],
            recv_sem=raw_recv.at[ci],
            device_id={"tm": partner},
            device_id_type=MESH,
        )

    def halo_copy(ci):
        return pltpu.make_async_remote_copy(
            src_ref=away.at[ci, side],
            dst_ref=work.at[ci, 5 * (1 - side)],
            send_sem=halo_send.at[ci],
            recv_sem=halo_recv.at[ci],
            device_id={"tm": lax.clamp(0, across, times - 1)},
            device_id_type=MESH,
        )

    def mask_copy(k):
        return pltpu.make_async_remote_copy(
            src_ref=masks.at[me],
            dst_ref=masks.at[me],
            send_sem=mask_send.at[k],
            recv_sem=mask_recv.at[me],
            device_id={"tm": lax.rem(me + k, times)},
            device_id_type=MESH,
        )

    def owner_copy(k, slot):
        return pltpu.make_async_remote_copy(
            src_ref=owners.at[slot],
            dst_ref=owners.at[slot],
            send_sem=owner_send.at[k],
            recv_sem=owner_recv.at[slot],
            device_id=peer(k),
            device_id_type=MESH,
        )

    def mean_copy(k, slot, ci):
        return pltpu.make_async_remote_copy(
            src_ref=means.at[slot, ci],
            dst_ref=means.at[slot, ci],
            send_sem=mean_send.at[k, ci],
            recv_sem=mean_recv.at[slot, ci],
            device_id=peer(k),
            device_id_type=MESH,
        )

    toward = jnp.where(2 * me < times, times - 1, 1)

    def part_copy(k, ci, which):
        target = lax.rem(me + k * toward, times)
        return pltpu.make_async_remote_copy(
            src_ref=stage.at[target, ci, which],
            dst_ref=arrived.at[me, ci, which],
            send_sem=part_send.at[k, ci, which],
            recv_sem=part_recv.at[me, ci, which],
            device_id={"tm": target},
            device_id_type=MESH,
        )

    for k in range(1, times):
        mask_copy(k).start()
    for k in range(1, peers):
        owner_copy(k, mine).start()
    for ci in range(nh):
        raw_copy(ci).start()

        @pl.when(has_across)
        def _():
            halo_copy(ci).start()

    for k in range(1, times):
        source = lax.rem(me + k, times)
        pltpu.make_async_remote_copy(
            src_ref=masks.at[source],
            dst_ref=masks.at[source],
            send_sem=mask_send.at[k],
            recv_sem=mask_recv.at[source],
            device_id={"tm": source},
            device_id_type=MESH,
        ).wait_recv()

    for k in range(1, peers):
        owner_copy(k, lax.rem(mine + k, peers)).wait_recv()
    for one in copies[1:]:
        one.wait()

    lane = lax.broadcasted_iota(jnp.int32, (8, LB), 1)
    sub_row = lax.broadcasted_iota(jnp.int32, (8, LB), 0)
    swap = jnp.logical_and(sub_row == 0, lane >= LB // 2)
    mirror = lax.rem(LB - lax.broadcasted_iota(jnp.int32, (LB // 2, LB), 1), LB)

    def in_order(table):
        head = jnp.where(swap, jnp.broadcast_to(table[rows : rows + 1], (8, LB)), table[:8])
        turned = jnp.concatenate([head, table[8:rows]], axis=0).T
        back = jnp.take_along_axis(turned[LB // 2 :], mirror, axis=1)
        return jnp.concatenate([turned[: LB // 2], back], axis=1)

    def one_channel(ci, carry):
        raw_copy(ci).wait_recv()

        @pl.when(has_across)
        def _():
            halo_copy(ci).wait_recv()

        columns_high, columns_low = [], []
        for s in range(5):
            frame = jnp.concatenate(
                [work[ci, s] * window[0], work[ci, s + 1] * window[1]], axis=0
            )
            high, low = split_value(frame)
            columns_high.append(high)
            columns_low.append(low)
        frames = (jnp.concatenate(columns_high, axis=1), jnp.concatenate(columns_low, axis=1))
        middle = three_pass((one_high[...], one_low[...]), frames)
        real, imag = middle[: rows + 8], middle[rows + 8 :]
        cosine, sine = twiddle[0], twiddle[1]
        turned = []
        for s in range(5):
            re, im = real[:, s * LB : (s + 1) * LB], imag[:, s * LB : (s + 1) * LB]
            turned.append(
                jnp.concatenate([re * cosine - im * sine, re * sine + im * cosine], axis=1)
            )
        turned = jnp.concatenate(turned, axis=0)
        bins = three_pass(split_value(turned), (two_high[...], two_low[...]))
        powers = bins[:, :LB] * bins[:, :LB] + bins[:, LB:] * bins[:, LB:]
        channel = side * nh + ci
        owned = [jnp.float32(1.0)] * 5
        owned[0] = jnp.logical_and(side == 0, has_across).astype(F32)
        owned[4] = jnp.logical_or(side == 1, pair == pairs - 1).astype(F32)
        peak, product = None, None
        for s in range(5):
            holder = jnp.maximum(2 * pair + (s - 1) // 2, 0)
            keep = masks[holder, (s - 1) % 2, pl.ds(channel, 1), :] * owned[s] > 0.5
            here = powers[s * (rows + 8) : (s + 1) * (rows + 8)]
            held = jnp.where(keep, here, 0.0)
            factor = jnp.where(keep, here + 0.25, 1.0)
            peak = held if peak is None else jnp.maximum(peak, held)
            product = factor if product is None else product * factor
        for which, table in enumerate((peak, jnp.log(product))):
            ordered = in_order(table)
            for target in range(times):
                stage[target, ci, which] = ordered[target * out_rows : (target + 1) * out_rows]
        for k in range(1, times):
            part_copy(k, ci, 1).start()
        arrived[me, ci] = stage[me, ci]
        return carry

    lax.fori_loop(0, nh, one_channel, 0)
    for k in range(1, times):
        for ci in range(nh):
            part_copy(k, ci, 0).start()

    kept = jnp.zeros((channels, LB), F32)
    for t in range(times):
        kept = kept + masks[t, 0] + masks[t, 1]

    blocks = [jnp.zeros((out_rows, 2 * LB), F32) for _ in range(BLOCKS)]

    def add_means(blocks, slot, ci):
        for half in range(2):
            mean = means[slot, ci, half]
            row = owners[slot, half * nh + ci : half * nh + ci + 1, :]
            row = jnp.concatenate([row, row], axis=1)
            blocks = [total + mean * (row == b).astype(F32) for b, total in enumerate(blocks)]
        return blocks

    def await_parts(ci, which):
        for k in range(1, times):
            source = lax.rem(me + k, times)
            pltpu.make_async_remote_copy(
                src_ref=arrived.at[source, ci, which],
                dst_ref=arrived.at[source, ci, which],
                send_sem=part_send.at[k, ci, which],
                recv_sem=part_recv.at[source, ci, which],
                device_id={"tm": source},
                device_id_type=MESH,
            ).wait_recv()

    for ci in range(nh):
        await_parts(ci, 1)
        for half in range(2):
            c = half * nh + ci
            logs = arrived[half, ci, 1]
            for p in range(1, pairs):
                logs = logs + arrived[2 * p + half, ci, 1]
            row = kept[c : c + 1]
            mean = logs / jnp.concatenate([row, row], axis=1)
            mean_out[c] = mean
            means[mine, ci, half] = mean
        for k in range(1, peers):
            mean_copy(k, mine, ci).start()
        if ci > 0:
            for k in range(1, peers):
                mean_copy(k, lax.rem(mine + k, peers), ci - 1).wait_recv()
            for slot in range(peers):
                blocks = add_means(blocks, slot, ci - 1)
    for ci in range(nh):
        await_parts(ci, 0)
        for half in range(2):
            peak = arrived[half, ci, 0]
            for p in range(1, pairs):
                peak = jnp.maximum(peak, arrived[2 * p + half, ci, 0])
            peak_out[half * nh + ci] = peak
    sizes_of = []
    for b in range(BLOCKS):
        held = jnp.zeros((channels, LB), F32)
        for slot in range(peers):
            held = held + (owners[slot] == b).astype(F32)
        size = jnp.sum(held, axis=0, keepdims=True)
        sizes_of.append(jnp.concatenate([size, size], axis=1))
    for k in range(1, peers):
        mean_copy(k, lax.rem(mine + k, peers), nh - 1).wait_recv()
    for slot in range(peers):
        blocks = add_means(blocks, slot, nh - 1)
    for b in range(BLOCKS):
        block_out[b] = blocks[b] / sizes_of[b]

    for k in range(1, peers):
        owner_copy(k, mine).wait_send()
        for ci in range(nh):
            mean_copy(k, mine, ci).wait_send()
    for k in range(1, times):
        mask_copy(k).wait_send()
    for ci in range(nh):
        raw_copy(ci).wait_send()

        @pl.when(has_across)
        def _():
            halo_copy(ci).wait_send()

        for k in range(1, times):
            for which in range(2):
                part_copy(k, ci, which).wait_send()


def flatten(*refs):
    for lines, flat in zip(refs[:3], refs[3:]):
        for j in range(lines.shape[1]):
            for half in range(2):
                at = (2 * j + half) * LB
                flat[:, at : at + LB] = lines[:, j, half * LB : (half + 1) * LB]


def on_device(sizes, signal, gap_mask, assignment):
    times, subs, chans = sizes
    channels, local_time = signal.shape
    nh = channels // 2
    rows = LA // 2
    width = LA * LB // 2 // times
    out_rows = width // (2 * LB)
    peers = subs * chans
    constants = [jnp.asarray(t) for t in tables()]
    vmem = pl.BlockSpec(memory_space=pltpu.VMEM)
    smem = pl.BlockSpec(memory_space=pltpu.SMEM)
    hbm = pl.BlockSpec(memory_space=pl.ANY)
    dma = pltpu.SemaphoreType.DMA
    inputs = [signal, *constants]
    lines = [(channels, out_rows, 2 * LB)] * 2 + [(BLOCKS, out_rows, 2 * LB)]
    found = pl.pallas_call(
        functools.partial(kernel, sizes),
        out_shape=[pltpu.VMEM(shape, F32) for shape in lines],
        in_specs=[smem, hbm, smem] + [hbm] * 6,
        out_specs=[vmem] * 3,
        scratch_shapes=[
            *[pltpu.VMEM(one.shape, one.dtype) for one in inputs],
            pltpu.VMEM((nh, 6, rows, LB), F32),
            pltpu.VMEM((nh, 2, rows, LB), F32),
            pltpu.VMEM((times, nh, 2, out_rows, 2 * LB), F32),
            pltpu.VMEM((times, nh, 2, out_rows, 2 * LB), F32),
            pltpu.VMEM((times, 2, channels, LB), F32),
            pltpu.VMEM((peers, nh, 2, out_rows, 2 * LB), F32),
            pltpu.VMEM((peers, channels, LB), F32),
            dma((len(inputs),)),
            dma((nh,)),
            dma((nh,)),
            dma((nh,)),
            dma((nh,)),
            dma((times,)),
            dma((times,)),
            dma((times, nh, 2)),
            dma((times, nh, 2)),
            dma((peers, nh)),
            dma((peers, nh)),
            dma((peers,)),
            dma((peers,)),
        ],
        compiler_params=pltpu.CompilerParams(collective_id=0, has_side_effects=True),
    )(assignment, signal, gap_mask.T, *constants)
    return pl.pallas_call(
        flatten,
        out_shape=[jax.ShapeDtypeStruct((shape[0], width), F32) for shape in lines],
        in_specs=[vmem] * 3,
        out_specs=[vmem] * 3,
    )(*[pltpu.with_memory_space_constraint(one, pltpu.VMEM) for one in found])


def solution(mesh):
    sizes = (mesh.shape["tm"], mesh.shape["sub"], mesh.shape["chan"])
    in_specs = (
        P(("grp", "chan", "sub"), "tm"),
        P(("grp", "chan", "sub"), "tm"),
        P(("grp", "chan", "sub")),
    )
    out_specs = (P(("grp", "chan", "sub"), "tm"), P(("grp", "chan", "sub"), "tm"), P("grp", "tm"))
    return jax.shard_map(
        functools.partial(on_device, sizes),
        mesh=mesh,
        in_specs=in_specs,
        out_specs=out_specs,
        check_vma=False,
    )
```
